32 devices in a mesh: data: 2 (over x), tp: 4 (over z), ep: 4 (over y, core).
Axes of the slice: x: 2, y: 2, z: 4, core: 2. Of those that a mesh axis runs over, the one named last changes fastest.
Arguments:
- tokens: bfloat16 [8192, 2048], P(('data', 'ep', 'tp')), parts along dimension 0
- expert_ids: int32 [8192, 6], P(('data', 'ep', 'tp')), parts along dimension 0
- gate_vals: float32 [8192, 6], P(('data', 'ep', 'tp')), parts along dimension 0
- slot_ids: int32 [8192, 6], P(('data', 'ep', 'tp')), parts along dimension 0
- send_counts: int32 [32, 64], P(('data', 'ep', 'tp')), parts along dimension 0
- shared_w1: bfloat16 [2048, 2816], P(None, 'tp')
- shared_w3: bfloat16 [2048, 2816], P(None, 'tp')
- shared_w2: bfloat16 [2816, 2048], P('tp')
- expert_w1: bfloat16 [64, 2048, 1408], P('ep')
- expert_w3: bfloat16 [64, 2048, 1408], P('ep')
- expert_w2: bfloat16 [64, 1408, 2048], P('ep')
Outputs:
- output: bfloat16 [8192, 2048], P(('data', 'ep', 'tp')), parts along dimension 0
There are 2 independent parts. The reference program is written for one: setup_inputs(seed, part) draws one part's arguments, and reference() takes and returns one part's arrays. A program takes and returns all parts, laid end to end along the dimension named above; an argument that names none is the same for every part.
All inputs are finite; a program needn't handle non-finite values.
Results may differ from the reference program's by a relative error of at most 0.00128.
Values are sent between devices in bfloat16 or wider.
A program may use at most 1.25 GiB of HBM per device.

```python
import jax
import jax.numpy as jnp
from jax import lax

EP = 4
TP = 4
TOKENS_DEV = 256
D = 2048
FS = 2816
FF = 1408
EXPERTS = 64
TOP = 6
HOT = 8
CAP = 96

N_SRC = EP * TP
TOKENS = TOKENS_DEV * N_SRC


def draw_routing(route_key):
    key_hot, key_wts, key_perm = jax.random.split(route_key, 3)
    experts = jnp.arange(EXPERTS, dtype=jnp.int32)
    offset = jax.random.randint(key_hot, (), 0, EXPERTS, dtype=jnp.int32)
    is_hot = ((experts - offset) % EXPERTS) < HOT
    weights = jax.random.randint(key_wts, (N_SRC, EXPERTS), 1, 3, dtype=jnp.int32)
    cum_wts = jnp.cumsum(jnp.where(is_hot[None, :], 0, weights), axis=1)
    cold_total = TOKENS_DEV * TOP - HOT * CAP
    bounds = (cold_total * cum_wts) // cum_wts[:, -1:]
    prev_bounds = jnp.concatenate([jnp.zeros((N_SRC, 1), jnp.int32), bounds[:, :-1]], axis=1)
    counts = jnp.where(is_hot[None, :], CAP, bounds - prev_bounds).astype(jnp.int32)
    run_ends = jnp.cumsum(counts, axis=1)
    copy_pos = jnp.arange(TOKENS_DEV * TOP, dtype=jnp.int32)
    expert_of = jax.vmap(lambda end_row: jnp.searchsorted(end_row, copy_pos, side="right"))(run_ends).astype(jnp.int32)
    slot_of = copy_pos[None, :] - jnp.take_along_axis(run_ends - counts, expert_of, axis=1)
    expert_of = expert_of.reshape(N_SRC, TOP, TOKENS_DEV).transpose(0, 2, 1)
    slot_of = slot_of.reshape(N_SRC, TOP, TOKENS_DEV).transpose(0, 2, 1)
    tok_perms = jax.vmap(lambda perm_key: jax.random.permutation(perm_key, TOKENS_DEV))(jax.random.split(key_perm, N_SRC))
    expert_of = jnp.take_along_axis(expert_of, tok_perms[:, :, None], axis=1)
    slot_of = jnp.take_along_axis(slot_of, tok_perms[:, :, None], axis=1)
    return expert_of.reshape(TOKENS, TOP).astype(jnp.int32), slot_of.reshape(TOKENS, TOP).astype(jnp.int32), counts


def scaled_normal(weight_key, shape, fan_in):
    return (jax.random.normal(weight_key, shape, jnp.float32) * fan_in ** -0.5).astype(jnp.bfloat16)


def setup_inputs(seed: int = 0, part: int = 0) -> dict:
    base_key = jax.random.key(seed)
    part_key = jax.random.fold_in(base_key, part)
    key_x, key_gate, key_route = jax.random.split(part_key, 3)
    weight_keys = jax.random.split(jax.random.key(seed + 1), 6)
    tokens = jax.random.normal(key_x, (TOKENS, D), jnp.float32).astype(jnp.bfloat16)
    expert_ids, slot_ids, send_counts = draw_routing(key_route)
    gate_vals = jax.random.uniform(key_gate, (TOKENS, TOP), jnp.float32, 0.5, 1.5) * TOP ** -0.5
    return {
        "tokens": tokens,
        "expert_ids": expert_ids,
        "gate_vals": gate_vals,
        "slot_ids": slot_ids,
        "send_counts": send_counts,
        "shared_w1": scaled_normal(weight_keys[0], (D, FS), D),
        "shared_w3": scaled_normal(weight_keys[1], (D, FS), D),
        "shared_w2": scaled_normal(weight_keys[2], (FS, D), FS),
        "expert_w1": scaled_normal(weight_keys[3], (EXPERTS, D, FF), D),
        "expert_w3": scaled_normal(weight_keys[4], (EXPERTS, D, FF), D),
        "expert_w2": scaled_normal(weight_keys[5], (EXPERTS, FF, D), FF),
    }


def shared_block(tok_block, shared_w1, shared_w3, shared_w2):
    pre_gate = jnp.dot(tok_block, shared_w1, preferred_element_type=jnp.float32)
    pre_up = jnp.dot(tok_block, shared_w3, preferred_element_type=jnp.float32)
    hidden = (jax.nn.silu(pre_gate) * pre_up).astype(jnp.bfloat16)
    return jnp.dot(hidden, shared_w2, preferred_element_type=jnp.float32)


def reference(tokens, expert_ids, gate_vals, slot_ids, send_counts, shared_w1, shared_w3, shared_w2, expert_w1, expert_w3, expert_w2):
    tok_blocks = tokens.reshape(N_SRC, TOKENS_DEV, D)
    shared_out = lax.map(lambda tok_block: shared_block(tok_block, shared_w1, shared_w3, shared_w2), tok_blocks).reshape(TOKENS, D)
    src_ids = jnp.arange(TOKENS, dtype=jnp.int32) // TOKENS_DEV
    row_limit = send_counts[src_ids[:, None], expert_ids]
    kept_mask = (slot_ids >= 0) & (slot_ids < row_limit)
    n_rows = N_SRC * EXPERTS * CAP
    dest_row = jnp.where(kept_mask, (src_ids[:, None] * EXPERTS + expert_ids) * CAP + slot_ids, n_rows)
    copy_ids = jnp.arange(TOKENS * TOP, dtype=jnp.int32)
    owner_ids = jnp.full((n_rows,), TOKENS * TOP, jnp.int32).at[dest_row.reshape(-1)].set(copy_ids, mode="drop")
    owner_ids = owner_ids.reshape(N_SRC, EXPERTS, CAP).transpose(1, 0, 2).reshape(EXPERTS, N_SRC * CAP)
    flat_gates = gate_vals.reshape(-1)

    def expert_step(running, step_in):
        w_in, w_up, w_out, own_ids = step_in
        tok_of = own_ids // TOP
        expert_rows = jnp.take(tokens, tok_of, axis=0, mode="fill", fill_value=0)
        pre_gate = jnp.dot(expert_rows, w_in, preferred_element_type=jnp.float32)
        pre_up = jnp.dot(expert_rows, w_up, preferred_element_type=jnp.float32)
        hidden = (jax.nn.silu(pre_gate) * pre_up).astype(jnp.bfloat16)
        routed = jnp.dot(hidden, w_out, preferred_element_type=jnp.float32).astype(jnp.bfloat16)
        weight = jnp.take(flat_gates, own_ids, mode="fill", fill_value=0)
        running = running.at[tok_of].add(weight[:, None] * routed.astype(jnp.float32), mode="drop")
        return running, None

    routed_sum = lax.scan(expert_step, jnp.zeros((TOKENS, D), jnp.float32), (expert_w1, expert_w3, expert_w2, owner_ids))[0]
    return (tokens.astype(jnp.float32) + shared_out + routed_sum).astype(jnp.bfloat16)
```

```python
import functools

import jax
import jax.numpy as jnp
from jax import lax
from jax.experimental import pallas as pl
from jax.experimental.pallas import tpu as pltpu
from jax.sharding import PartitionSpec as P

CAP_FACTOR = 4
GROUP = 4
N_CHUNKS = 2
VMEM_LIMIT = 66_000_000


def capacity_rows(n_tok, top_k, n_exp):
    return min(n_tok, ((CAP_FACTOR * n_tok * top_k // n_exp + 7) // 8) * 8)


def row_sizes(rows):
    return [size for size in (128, 256) if size < rows] + [rows]


def pick_rows(n_rows, rows, body):
    low = 0
    for size in row_sizes(rows):
        high = size if size < rows else rows + 1
        pl.when((n_rows > low if low else n_rows >= 0) & (n_rows <= high))(functools.partial(body, size))
        low = size


def column_pieces(width, step):
    pieces, start = [], 0
    while start < width:
        size = min(step, width - start)
        pieces.append((start, size))
        start += size
    return pieces


def up_kernel(cap, off_ref, n_ref, pick_ref, x0_ref, x1_ref, x2_ref, x3_ref, w1_ref, w3_ref, h_ref, rows_ref):
    step = pl.program_id(0)
    rows = h_ref.shape[1]
    d_model = x0_ref.shape[1]
    d_ff = w1_ref.shape[2]
    x_refs = (x0_ref, x1_ref, x2_ref, x3_ref)

    @pl.when(step % GROUP == 0)
    def _():
        for src, x_ref in enumerate(x_refs):
            chosen = pick_ref[src]
            for start, size in column_pieces(d_model, 512):
                got = jnp.dot(chosen, x_ref[:, start : start + size], preferred_element_type=jnp.float32).astype(jnp.bfloat16)
                for part in range(GROUP):
                    at = pl.multiple_of(off_ref[(step + part) * 4 + src], 16)
                    rows_ref[part, pl.ds(at, cap), start : start + size] = got[part * cap : (part + 1) * cap]

    part = step % GROUP

    def body(size):
        x = rows_ref[part, :size, :]
        full = d_ff // 256 * 256
        for start, width in column_pieces(full, 512):
            gate = jnp.dot(x, w1_ref[0, :, start : start + width], preferred_element_type=jnp.float32)
            up = jnp.dot(x, w3_ref[0, :, start : start + width], preferred_element_type=jnp.float32)
            h_ref[0, :size, start : start + width] = (jax.nn.silu(gate) * up).astype(jnp.bfloat16)
        if full < d_ff:
            tail = d_ff - full
            both = jnp.concatenate([w1_ref[0, :, full:], w3_ref[0, :, full:]], axis=1)
            pair = jnp.dot(x, both, preferred_element_type=jnp.float32)
            h_ref[0, :size, full:] = (jax.nn.silu(pair[:, :tail]) * pair[:, tail:]).astype(jnp.bfloat16)

    pick_rows(n_ref[step], rows, body)


def down_kernel(cap, off_ref, n_ref, queue_off_ref, total_ref, h_ref, w2_ref, gates_ref, own_ref, sib_ref, out_ref, queue_ref):
    step = pl.program_id(0)
    n_local = pl.num_programs(0)
    rows = h_ref.shape[1]
    width_all = w2_ref.shape[2]
    n_queue = queue_ref.shape[1]

    def body(size):
        for start, width in column_pieces(width_all, 512):
            out = jnp.dot(h_ref[0, :size, :], w2_ref[0, :, start : start + width], preferred_element_type=jnp.float32)
            out_ref[:size, start : start + width] = out.astype(jnp.bfloat16)

    pick_rows(n_ref[step], rows, body)
    for src in range(4):
        at = pl.multiple_of(off_ref[step * 4 + src], 16)
        to = pl.multiple_of(queue_off_ref[src * n_local + step], 16)
        queue_ref[src, pl.ds(to, cap), :] = out_ref[pl.ds(at, cap), :]

    @pl.when(step == n_local - 1)
    def _():
        for src in range(4):
            total = total_ref[src]
            n_tiles = (total + 255) // 256

            def clear(piece, carry):
                at = pl.multiple_of(total + piece * 16, 16)
                queue_ref[src, pl.ds(at, 16), :] = jnp.zeros((16, width_all), jnp.bfloat16)
                return carry

            lax.fori_loop(0, (n_tiles * 256 - total) // 16, clear, 0)
            into = (own_ref, sib_ref, own_ref, sib_ref)[src]
            place = src // 2
            into[place] = jnp.zeros(into.shape[1:], jnp.float32)

            def add(tile, carry):
                at = pl.multiple_of(tile * 256, 256)
                for start, width in column_pieces(width_all, 512):
                    held = queue_ref[src, pl.ds(at, 256), start : start + width]
                    new = into[place, :, start : start + width]
                    for piece in range(3):
                        new += jnp.dot(gates_ref[piece, src, :, pl.ds(at, 256)], held, preferred_element_type=jnp.float32)
                    into[place, :, start : start + width] = new
                return carry

            lax.fori_loop(0, n_tiles, add, 0)


def solution(mesh):
    ep_size = mesh.shape["ep"]
    row_spec = P(("data", "ep", "tp"), None)
    expert_spec = P("ep", None, None)
    n_rep = mesh.shape["data"] * ep_size

    def layer_body(tokens, expert_ids, gate_vals, slot_ids, send_counts, shared_w1, shared_w3, shared_w2, expert_w1, expert_w3, expert_w2):
        n_tok, d_model = tokens.shape
        top_k = expert_ids.shape[1]
        n_local, _, d_ff = expert_w1.shape
        n_exp = n_local * ep_size
        cap = capacity_rows(n_tok, top_k, n_exp)
        rows = ep_size * cap
        n_queue = n_local * cap
        me = lax.axis_index("ep")

        def swap(value, bit):
            return lax.ppermute(value, "ep", [(i, i ^ bit) for i in range(ep_size)])

        all_ids = jnp.arange(n_exp, dtype=jnp.int32)
        row_limit = jnp.sum(jnp.where(expert_ids[:, :, None] == all_ids, send_counts[0], 0), axis=-1)
        kept_mask = (slot_ids >= 0) & (slot_ids < row_limit)
        dest_row = jnp.where(kept_mask, expert_ids * cap + slot_ids, -1)
        facts = jnp.concatenate(
            [
                dest_row.astype(jnp.float32).T,
                jnp.where(kept_mask, gate_vals, 0.0).T,
                jnp.pad(send_counts.astype(jnp.float32), ((0, 0), (0, n_tok - n_exp))),
                jnp.zeros((15 - 2 * top_k, n_tok), jnp.float32),
            ],
            axis=0,
        )

        facts_sib = swap(facts, 1)
        facts_far = swap(facts, 2)
        x_far = swap(tokens, 2)
        x_sib = swap(tokens, 1)
        facts_all = jnp.stack([facts, facts_sib, facts_far, swap(facts_far, 1)])
        x_far_sib = swap(x_far, 1)

        dest_all = facts_all[:, :top_k].astype(jnp.int32) - me * n_queue
        dest_all = jnp.where((dest_all >= 0) & (dest_all < n_queue), dest_all, -1)
        gates_all = facts_all[:, top_k : 2 * top_k]
        counts_all = lax.dynamic_slice_in_dim(facts_all[:, 2 * top_k], me * n_local, n_local, 1).astype(jnp.int32)
        padded = (counts_all + 15) // 16 * 16
        off = (jnp.cumsum(padded, axis=0) - padded).T.reshape(-1)
        n_rows = jnp.sum(padded, axis=0)
        queue_off = jnp.cumsum(padded, axis=1) - padded
        total = jnp.sum(padded, axis=1)

        lanes = jnp.arange(n_queue, dtype=jnp.int32)
        pick = jnp.any(dest_all[:, :, None, :] == lanes[:, None], axis=1).astype(jnp.bfloat16)
        local = jnp.arange(n_local, dtype=jnp.int32)
        shift = jnp.sum(jnp.where((dest_all // cap)[..., None] == local, (queue_off - local * cap)[:, None, None, :], 0), axis=-1)
        queue_row = jnp.where(dest_all >= 0, dest_all + shift, -1).transpose(0, 2, 1)
        high = lax.reduce_precision(gates_all, 8, 7)
        middle = lax.reduce_precision(gates_all - high, 8, 7)
        low = lax.reduce_precision(gates_all - high - middle, 8, 7)
        pieces = jnp.stack([high, middle, low]).transpose(0, 1, 3, 2)
        gate_rows = jnp.sum(
            jnp.where(queue_row[..., None] == lanes, pieces[..., None], 0.0), axis=3
        ).astype(jnp.bfloat16)

        whole = dict(pipeline_mode=pl.Buffered(1))
        hidden = pl.pallas_call(
            functools.partial(up_kernel, cap),
            grid_spec=pltpu.PrefetchScalarGridSpec(
                num_scalar_prefetch=2,
                grid=(n_local,),
                in_specs=[
                    pl.BlockSpec((4, GROUP * cap, n_tok), lambda e, *_: (0, e // GROUP, 0)),
                    *[pl.BlockSpec((n_tok, d_model), lambda e, *_: (0, 0), **whole) for _ in range(4)],
                    pl.BlockSpec((1, d_model, d_ff), lambda e, *_: (e, 0, 0)),
                    pl.BlockSpec((1, d_model, d_ff), lambda e, *_: (e, 0, 0)),
                ],
                out_specs=pl.BlockSpec((1, rows, d_ff), lambda e, *_: (e, 0, 0)),
                scratch_shapes=[pltpu.VMEM((GROUP, rows, d_model), jnp.bfloat16)],
            ),
            out_shape=jax.ShapeDtypeStruct((n_local, rows, d_ff), jnp.bfloat16),
            compiler_params=pltpu.CompilerParams(dimension_semantics=("arbitrary",), vmem_limit_bytes=VMEM_LIMIT),
            cost_estimate=pl.CostEstimate(flops=4 * n_local * 192 * d_model * d_ff, bytes_accessed=4 * n_local * d_model * d_ff, transcendentals=0),
            name="experts_up",
        )(off, n_rows, pick, tokens, x_sib, x_far, x_far_sib, expert_w1, expert_w3)

        gathered = lax.all_gather(tokens, "tp", axis=0, tiled=True)
        gathered, hidden = lax.optimization_barrier((gathered, hidden))
        pre_gate = jnp.dot(gathered, shared_w1, preferred_element_type=jnp.float32)
        pre_up = jnp.dot(gathered, shared_w3, preferred_element_type=jnp.float32)
        shared_hidden = (jax.nn.silu(pre_gate) * pre_up).astype(jnp.bfloat16)
        shared_hidden, hidden = lax.optimization_barrier((shared_hidden, hidden))
        hidden_blocks = lax.all_to_all(shared_hidden.reshape(mesh.shape["tp"], n_tok, -1), "tp", 0, 0)

        width = shared_w2.shape[0]
        rep = lax.axis_index("data") * ep_size + me
        w2_part = lax.dynamic_slice_in_dim(shared_w2, rep * (width // n_rep), width // n_rep, 0)
        w2_all = lax.all_gather(w2_part, ("tp", "data", "ep"), axis=0, tiled=True)

        n_cols = d_model // N_CHUNKS
        routed = []
        for chunk in range(N_CHUNKS):
            sums_own, sums_sib = pl.pallas_call(
                functools.partial(down_kernel, cap),
                grid_spec=pltpu.PrefetchScalarGridSpec(
                    num_scalar_prefetch=4,
                    grid=(n_local,),
                    in_specs=[
                        pl.BlockSpec((1, rows, d_ff), lambda e, *_: (e, 0, 0)),
                        pl.BlockSpec((1, d_ff, n_cols), functools.partial(lambda c, e, *_: (e, 0, c), chunk)),
                        pl.BlockSpec((3, 4, n_tok, n_queue), lambda e, *_: (0, 0, 0, 0), **whole),
                    ],
                    out_specs=[pl.BlockSpec((2, n_tok, n_cols), lambda e, *_: (0, 0, 0), **whole) for _ in range(2)],
                    scratch_shapes=[pltpu.VMEM((rows, n_cols), jnp.bfloat16), pltpu.VMEM((4, n_queue, n_cols), jnp.bfloat16)],
                ),
                out_shape=[jax.ShapeDtypeStruct((2, n_tok, n_cols), jnp.float32) for _ in range(2)],
                compiler_params=pltpu.CompilerParams(dimension_semantics=("arbitrary",), vmem_limit_bytes=VMEM_LIMIT),
                cost_estimate=pl.CostEstimate(flops=2 * n_local * 192 * n_cols * d_ff, bytes_accessed=2 * n_local * n_cols * d_ff, transcendentals=0),
                name=f"experts_down_{chunk}",
            )(off, n_rows, queue_off.reshape(-1), total, hidden, expert_w2, gate_rows)
            from_sib = swap(sums_sib, 1)
            from_far = swap(sums_own[1] + from_sib[1], 2)
            routed.append(sums_own[0] + from_sib[0] + from_far)
        routed_sum = jnp.concatenate(routed, axis=1)

        w2_blocks = w2_all.reshape(mesh.shape["tp"], width, d_model)
        shared_out = jnp.dot(hidden_blocks[0], w2_blocks[0], preferred_element_type=jnp.float32)
        for block in range(1, mesh.shape["tp"]):
            shared_out += jnp.dot(hidden_blocks[block], w2_blocks[block], preferred_element_type=jnp.float32)
        return (tokens.astype(jnp.float32) + shared_out + routed_sum).astype(jnp.bfloat16)

    return jax.shard_map(
        layer_body,
        mesh=mesh,
        in_specs=(row_spec, row_spec, row_spec, row_spec, row_spec, P(None, "tp"), P(None, "tp"), P("tp", None), expert_spec, expert_spec, expert_spec),
        out_specs=row_spec,
        check_vma=False,
    )
```

```python
import functools

import jax
import jax.numpy as jnp
from jax import lax
from jax.experimental import pallas as pl
from jax.experimental.pallas import tpu as pltpu
from jax.sharding import PartitionSpec as P


CAP_FACTOR = 4
GROUP = 4
COLUMN_CHUNKS = 2
ROW_PIECE = 128
UP_SLOTS = 3
DOWN_SLOTS = 4
VMEM_LIMIT = 66_000_000


def capacity_rows(n_tok, top_k, n_exp):
    return min(n_tok, ((CAP_FACTOR * n_tok * top_k // n_exp + 7) // 8) * 8)


def row_sizes(rows):
    return [size for size in (128, 256) if size < rows] + [rows]


def pick_rows(n_rows, rows, body):
    low = 0
    for size in row_sizes(rows):
        high = size if size < rows else rows + 1
        pl.when((n_rows > low if low else n_rows >= 0) & (n_rows <= high))(functools.partial(body, size))
        low = size


def column_pieces(width, step):
    pieces, start = [], 0
    while start < width:
        size = min(step, width - start)
        pieces.append((start, size))
        start += size
    return pieces


def prep_kernel(facts_ref, gates_in_ref, pick_ref, gates_ref):
    top_k = gates_in_ref.shape[2]
    n_tok = pick_ref.shape[2]
    step_rows = 32

    def fill(block, carry):
        at = pl.multiple_of(block * step_rows, step_rows)
        row = lax.broadcasted_iota(jnp.int32, (step_rows, n_tok), 0) + at
        chosen = jnp.zeros((step_rows, n_tok), jnp.float32)
        for j in range(top_k):
            chosen = jnp.where(facts_ref[0, j : j + 1, :] == row, 1.0, chosen)
        pick_ref[0, pl.ds(at, step_rows), :] = chosen.astype(jnp.bfloat16)
        return carry

    lax.fori_loop(0, pick_ref.shape[1] // step_rows, fill, 0)

    def tile(index, carry):
        row = lax.broadcasted_iota(jnp.int32, (256, n_tok), 0) + index * 256
        for piece in range(3):
            weight = jnp.zeros((256, n_tok), jnp.float32)
            for j in range(top_k):
                weight = jnp.where(facts_ref[0, 8 + j : 9 + j, :] == row, gates_in_ref[piece, 0, j : j + 1, :], weight)
            gates_ref[index, piece] = weight.astype(jnp.bfloat16).T
        return carry

    lax.fori_loop(0, gates_ref.shape[0], tile, 0)


def up_kernel(cap, off_ref, n_ref, at1_ref, at2_ref, pick_ref, x0_ref, x1_ref, x2_ref, x3_ref, w1_hbm, w3_hbm, h0_ref, h1_ref, h2_ref, rows_ref, w1_ring, w3_ring, sems):
    step = pl.program_id(0)
    n_steps = pl.num_programs(0)
    d_model = x0_ref.shape[1]
    d_ff = w1_ring.shape[2]
    n_slots = w1_ring.shape[0]
    x_refs = (x0_ref, x1_ref, x2_ref, x3_ref)
    h_refs = (h0_ref, h1_ref, h2_ref)

    def fetch(expert):
        slot = expert % n_slots
        return (
            pltpu.make_async_copy(w1_hbm.at[expert], w1_ring.at[slot], sems.at[0, slot]),
            pltpu.make_async_copy(w3_hbm.at[expert], w3_ring.at[slot], sems.at[1, slot]),
        )

    def start(expert):
        for copy in fetch(expert):
            copy.start()

    @pl.when(step == 0)
    def _():
        for expert in range(n_slots - 1):
            start(expert)

    @pl.when(step + n_slots - 1 < n_steps)
    def _():
        start(step + n_slots - 1)

    @pl.when(step % GROUP == 0)
    def _():
        for src, x_ref in enumerate(x_refs):
            chosen = pick_ref[src]
            for begin, size in column_pieces(d_model, 512):
                got = jnp.dot(chosen, x_ref[:, begin : begin + size], preferred_element_type=jnp.float32).astype(jnp.bfloat16)
                for part in range(GROUP):
                    at = pl.multiple_of(off_ref[(step + part) * 4 + src], 16)
                    rows_ref[part, pl.ds(at, cap), begin : begin + size] = got[part * cap : (part + 1) * cap]

    part = step % GROUP
    slot = step % n_slots
    for copy in fetch(step):
        copy.wait()

    def body(size):
        x = rows_ref[part, :size, :]

        def put(value, begin, width):
            for piece in range(size // ROW_PIECE):
                h_refs[piece][0, :, begin : begin + width] = value[piece * ROW_PIECE : (piece + 1) * ROW_PIECE]

        full = d_ff // 256 * 256
        for begin, width in column_pieces(full, 512):
            gate = jnp.dot(x, w1_ring[slot, :, begin : begin + width], preferred_element_type=jnp.float32)
            up = jnp.dot(x, w3_ring[slot, :, begin : begin + width], preferred_element_type=jnp.float32)
            put((jax.nn.silu(gate) * up).astype(jnp.bfloat16), begin, width)
        if full < d_ff:
            tail = d_ff - full
            both = jnp.concatenate([w1_ring[slot, :, full:], w3_ring[slot, :, full:]], axis=1)
            pair = jnp.dot(x, both, preferred_element_type=jnp.float32)
            put((jax.nn.silu(pair[:, :tail]) * pair[:, tail:]).astype(jnp.bfloat16), full, tail)

    pick_rows(n_ref[step], rows_ref.shape[1], body)


def down_kernel(cap, first, off_ref, n_ref, queue_off_ref, total_ref, at1_ref, at2_ref, h0_ref, h1_ref, h2_ref, w2_hbm, gates_hbm, own_ref, sib_ref, out_ref, queue_ref, w2_ring, gates_ref, w_sems, gate_sems):
    step = pl.program_id(0)
    n_local = pl.num_programs(0)
    n_slots, _, width_all = w2_ring.shape
    n_tiles_max = gates_ref.shape[0] // 4
    h_refs = (h0_ref, h1_ref, h2_ref)

    def fetch(expert):
        slot = expert % n_slots
        return pltpu.make_async_copy(w2_hbm.at[expert, :, first : first + width_all], w2_ring.at[slot], w_sems.at[slot])

    def gate_copies(act):
        for src in range(4):
            for tile in range(n_tiles_max):
                index = src * n_tiles_max + tile
                copy = pltpu.make_async_copy(gates_hbm.at[index], gates_ref.at[index], gate_sems.at[index])
                pl.when(tile * 256 < total_ref[src])(functools.partial(act, copy))

    @pl.when(step == 0)
    def _():
        for expert in range(n_slots - 1):
            fetch(expert).start()
        gate_copies(lambda copy: copy.start())

    @pl.when(step + n_slots - 1 < n_local)
    def _():
        fetch(step + n_slots - 1).start()

    fetch(step).wait()
    slot = step % n_slots

    def body(size):
        h = jnp.concatenate([h_refs[piece][0] for piece in range(size // ROW_PIECE)], axis=0)
        for begin, width in column_pieces(width_all, 512):
            out = jnp.dot(h, w2_ring[slot, :, begin : begin + width], preferred_element_type=jnp.float32)
            out_ref[:size, begin : begin + width] = out.astype(jnp.bfloat16)

    pick_rows(n_ref[step], out_ref.shape[0], body)
    for src in range(4):
        at = pl.multiple_of(off_ref[step * 4 + src], 16)
        to = pl.multiple_of(queue_off_ref[src * n_local + step], 16)
        queue_ref[src, pl.ds(to, cap), :] = out_ref[pl.ds(at, cap), :]

    @pl.when(step == n_local - 1)
    def _():
        gate_copies(lambda copy: copy.wait())
        for src in range(4):
            total = total_ref[src]
            n_tiles = (total + 255) // 256

            def clear(piece, carry):
                at = pl.multiple_of(total + piece * 16, 16)
                queue_ref[src, pl.ds(at, 16), :] = jnp.zeros((16, width_all), jnp.bfloat16)
                return carry

            lax.fori_loop(0, (n_tiles * 256 - total) // 16, clear, 0)
            into = (own_ref, sib_ref, own_ref, sib_ref)[src]
            place = src // 2
            into[place] = jnp.zeros(into.shape[1:], jnp.float32)

            def add(tile, carry):
                at = pl.multiple_of(tile * 256, 256)
                for begin, width in column_pieces(width_all, 512):
                    held = queue_ref[src, pl.ds(at, 256), begin : begin + width]
                    new = into[place, :, begin : begin + width]
                    for piece in range(3):
                        new += jnp.dot(gates_ref[src * n_tiles_max + tile, piece], held, preferred_element_type=jnp.float32)
                    into[place, :, begin : begin + width] = new
                return carry

            lax.fori_loop(0, n_tiles, add, 0)


def solution(mesh):
    ep_size = mesh.shape["ep"]
    row_spec = P(("data", "ep", "tp"), None)
    expert_spec = P("ep", None, None)
    n_rep = mesh.shape["data"] * ep_size

    def layer_body(tokens, expert_ids, gate_vals, slot_ids, send_counts, shared_w1, shared_w3, shared_w2, expert_w1, expert_w3, expert_w2):
        n_tok, d_model = tokens.shape
        top_k = expert_ids.shape[1]
        n_local, _, d_ff = expert_w1.shape
        n_exp = n_local * ep_size
        cap = capacity_rows(n_tok, top_k, n_exp)
        rows = ep_size * cap
        n_queue = n_local * cap
        me = lax.axis_index("ep")

        def swap(value, bit):
            return lax.ppermute(value, "ep", [(i, i ^ bit) for i in range(ep_size)])

        x_far = swap(tokens, 2)
        x_sib = swap(tokens, 1)
        x_far_sib = swap(x_far, 1)
        all_ids = jnp.arange(n_exp, dtype=jnp.int32)
        row_limit = jnp.sum(jnp.where(expert_ids[:, :, None] == all_ids, send_counts[0], 0), axis=-1)
        kept_mask = (slot_ids >= 0) & (slot_ids < row_limit)
        dest_row = jnp.where(kept_mask, expert_ids * cap + slot_ids, -1)
        facts = jnp.concatenate(
            [
                dest_row.astype(jnp.float32).T,
                jnp.where(kept_mask, gate_vals, 0.0).T,
                jnp.pad(send_counts.astype(jnp.float32), ((0, 0), (0, n_tok - n_exp))),
                jnp.zeros((15 - 2 * top_k, n_tok), jnp.float32),
            ],
            axis=0,
        )
        facts_far = swap(facts, 2)
        facts_sib = swap(facts, 1)
        facts_all = jnp.stack([facts, facts_sib, facts_far, swap(facts_far, 1)])

        dest_all = facts_all[:, :top_k].astype(jnp.int32) - me * n_queue
        dest_all = jnp.where((dest_all >= 0) & (dest_all < n_queue), dest_all, -1)
        gates_all = facts_all[:, top_k : 2 * top_k]
        counts_all = lax.dynamic_slice_in_dim(facts_all[:, 2 * top_k], me * n_local, n_local, 1).astype(jnp.int32)
        padded = (counts_all + 15) // 16 * 16
        local = jnp.arange(n_local, dtype=jnp.int32)
        before = local[None, :] < local[:, None]
        queue_off = jnp.sum(jnp.where(before[None], padded[:, None, :], 0), axis=2)
        total = jnp.sum(padded, axis=1)
        src = jnp.arange(4, dtype=jnp.int32)
        off = jnp.sum(jnp.where((src[None, :] < src[:, None])[None], padded.T[:, None, :], 0), axis=2).reshape(-1)
        n_rows = jnp.sum(padded, axis=0)

        def piece_home(piece):
            need = n_rows > piece * ROW_PIECE
            last = jnp.max(jnp.where(need[None, :] & (local[None, :] <= local[:, None]), local[None, :], -1), axis=1)
            first = jnp.min(jnp.where(need, local, n_local))
            return jnp.where(last >= 0, last, jnp.where(first < n_local, first, 0))

        at1, at2 = piece_home(1), piece_home(2)
        shift = jnp.sum(jnp.where((dest_all // cap)[..., None] == local, (queue_off - local * cap)[:, None, None, :], 0), axis=-1)
        queue_row = jnp.where(dest_all >= 0, dest_all + shift, -1)
        pad_rows = jnp.full((4, 8 - top_k, n_tok), -1, jnp.int32)
        places = jnp.concatenate([dest_all, pad_rows, queue_row, pad_rows], axis=1)
        high = lax.reduce_precision(gates_all, 8, 7)
        middle = lax.reduce_precision(gates_all - high, 8, 7)
        low = lax.reduce_precision(gates_all - high - middle, 8, 7)
        n_tiles = n_queue // 256
        pick, gate_tiles = pl.pallas_call(
            prep_kernel,
            grid=(4,),
            in_specs=[
                pl.BlockSpec((1, 16, n_tok), lambda s: (s, 0, 0)),
                pl.BlockSpec((3, 1, top_k, n_tok), lambda s: (0, s, 0, 0)),
            ],
            out_specs=[
                pl.BlockSpec((1, n_queue, n_tok), lambda s: (s, 0, 0)),
                pl.BlockSpec((n_tiles, 3, n_tok, 256), lambda s: (s, 0, 0, 0)),
            ],
            out_shape=[
                jax.ShapeDtypeStruct((4, n_queue, n_tok), jnp.bfloat16),
                jax.ShapeDtypeStruct((4 * n_tiles, 3, n_tok, 256), jnp.bfloat16),
            ],
            compiler_params=pltpu.CompilerParams(dimension_semantics=("arbitrary",), vmem_limit_bytes=40_000_000),
            cost_estimate=pl.CostEstimate(flops=10**9, bytes_accessed=4 * n_queue * n_tok * 8, transcendentals=0),
            name="prep",
        )(places, jnp.stack([high, middle, low]))

        whole = dict(pipeline_mode=pl.Buffered(1))
        any_space = pl.BlockSpec(memory_space=pl.ANY)
        hidden = pl.pallas_call(
            functools.partial(up_kernel, cap),
            grid_spec=pltpu.PrefetchScalarGridSpec(
                num_scalar_prefetch=4,
                grid=(n_local,),
                in_specs=[
                    pl.BlockSpec((4, GROUP * cap, n_tok), lambda e, *_: (0, e // GROUP, 0)),
                    *[pl.BlockSpec((n_tok, d_model), lambda e, *_: (0, 0), **whole) for _ in range(4)],
                    any_space,
                    any_space,
                ],
                out_specs=[
                    pl.BlockSpec((1, ROW_PIECE, d_ff), lambda e, off, n, at1, at2: (e, 0, 0)),
                    pl.BlockSpec((1, ROW_PIECE, d_ff), lambda e, off, n, at1, at2: (at1[e], 0, 0)),
                    pl.BlockSpec((1, ROW_PIECE, d_ff), lambda e, off, n, at1, at2: (at2[e], 0, 0)),
                ],
                scratch_shapes=[
                    pltpu.VMEM((GROUP, rows, d_model), jnp.bfloat16),
                    pltpu.VMEM((UP_SLOTS, d_model, d_ff), jnp.bfloat16),
                    pltpu.VMEM((UP_SLOTS, d_model, d_ff), jnp.bfloat16),
                    pltpu.SemaphoreType.DMA((2, UP_SLOTS)),
                ],
            ),
            out_shape=[jax.ShapeDtypeStruct((n_local, ROW_PIECE, d_ff), jnp.bfloat16)] * 3,
            compiler_params=pltpu.CompilerParams(dimension_semantics=("arbitrary",), vmem_limit_bytes=VMEM_LIMIT),
            cost_estimate=pl.CostEstimate(flops=4 * n_local * 192 * d_model * d_ff, bytes_accessed=4 * n_local * d_model * d_ff, transcendentals=0),
            name="experts_up",
        )(off, n_rows, at1, at2, pick, tokens, x_sib, x_far, x_far_sib, expert_w1, expert_w3)

        n_cols = d_model // COLUMN_CHUNKS

        def down(chunk, held):
            return pl.pallas_call(
                functools.partial(down_kernel, cap, chunk * n_cols),
                grid_spec=pltpu.PrefetchScalarGridSpec(
                    num_scalar_prefetch=6,
                    grid=(n_local,),
                    in_specs=[
                        pl.BlockSpec((1, ROW_PIECE, d_ff), lambda e, *_: (e, 0, 0)),
                        pl.BlockSpec((1, ROW_PIECE, d_ff), lambda e, off, n, qo, tot, at1, at2: (at1[e], 0, 0)),
                        pl.BlockSpec((1, ROW_PIECE, d_ff), lambda e, off, n, qo, tot, at1, at2: (at2[e], 0, 0)),
                        any_space,
                        any_space,
                    ],
                    out_specs=[pl.BlockSpec((2, n_tok, n_cols), lambda e, *_: (0, 0, 0), **whole) for _ in range(2)],
                    scratch_shapes=[
                        pltpu.VMEM((rows, n_cols), jnp.bfloat16),
                        pltpu.VMEM((4, n_queue, n_cols), jnp.bfloat16),
                        pltpu.VMEM((DOWN_SLOTS, d_ff, n_cols), jnp.bfloat16),
                        pltpu.VMEM(gate_tiles.shape, jnp.bfloat16),
                        pltpu.SemaphoreType.DMA((DOWN_SLOTS,)),
                        pltpu.SemaphoreType.DMA((4 * n_tiles,)),
                    ],
                ),
                out_shape=[jax.ShapeDtypeStruct((2, n_tok, n_cols), jnp.float32) for _ in range(2)],
                compiler_params=pltpu.CompilerParams(dimension_semantics=("arbitrary",), vmem_limit_bytes=VMEM_LIMIT),
                cost_estimate=pl.CostEstimate(flops=2 * n_local * 192 * n_cols * d_ff, bytes_accessed=2 * n_local * n_cols * d_ff, transcendentals=0),
            )(off, n_rows, queue_off.reshape(-1), total, at1, at2, *held, expert_w2, gate_tiles)

        gathered = lax.all_gather(tokens, "tp", axis=0, tiled=True)
        sums_own, sums_sib, returned = [], [], []
        for chunk in range(COLUMN_CHUNKS):
            own, sib = down(chunk, hidden)
            from_sib = swap(sib, 1)
            if chunk == 0:
                gathered, own = lax.optimization_barrier((gathered, own))
                pre_gate = jnp.dot(gathered, shared_w1, preferred_element_type=jnp.float32)
                pre_up = jnp.dot(gathered, shared_w3, preferred_element_type=jnp.float32)
                shared_hidden = (jax.nn.silu(pre_gate) * pre_up).astype(jnp.bfloat16)
            passed_on = own[1] + from_sib[1]
            passed_on, shared_hidden, *hidden = lax.optimization_barrier((passed_on, shared_hidden, *hidden))
            returned.append(swap(passed_on, 2))
            if chunk == 0:
                hidden_blocks = lax.all_to_all(shared_hidden.reshape(mesh.shape["tp"], n_tok, -1), "tp", 0, 0)
            sums_own.append(own[0])
            sums_sib.append(from_sib[0])

        width = shared_w2.shape[0]
        rep = lax.axis_index("data") * ep_size + me
        w2_part = lax.dynamic_slice_in_dim(shared_w2, rep * (width // n_rep), width // n_rep, 0)
        w2_all = lax.all_gather(w2_part, ("tp", "data", "ep"), axis=0, tiled=True)
        w2_all, passed_on = lax.optimization_barrier((w2_all, passed_on))
        w2_blocks = w2_all.reshape(mesh.shape["tp"], width, d_model)
        shared_out = jnp.dot(hidden_blocks[0], w2_blocks[0], preferred_element_type=jnp.float32)
        for block in range(1, mesh.shape["tp"]):
            shared_out += jnp.dot(hidden_blocks[block], w2_blocks[block], preferred_element_type=jnp.float32)
        base = tokens.astype(jnp.float32) + shared_out
        parts = []
        for chunk in range(COLUMN_CHUNKS):
            routed = sums_own[chunk] + sums_sib[chunk] + returned[chunk]
            parts.append((base[:, chunk * n_cols : (chunk + 1) * n_cols] + routed).astype(jnp.bfloat16))
        return jnp.concatenate(parts, axis=1)


    return jax.shard_map(
        layer_body,
        mesh=mesh,
        in_specs=(row_spec, row_spec, row_spec, row_spec, row_spec, P(None, "tp"), P(None, "tp"), P("tp", None), expert_spec, expert_spec, expert_spec),
        out_specs=row_spec,
        check_vma=False,
    )
```

```python
import functools

import jax
import jax.numpy as jnp
from jax import lax
from jax.experimental import pallas as pl
from jax.experimental.pallas import tpu as pltpu
from jax.sharding import PartitionSpec as P


CAP_FACTOR = 4
GROUP = 4
COLUMN_CHUNKS = 2
ROW_PIECE = 128
UP_SLOTS = 3
DOWN_SLOTS = 4
VMEM_LIMIT = 66_000_000


def capacity_rows(n_tok, top_k, n_exp):
    return min(n_tok, ((CAP_FACTOR * n_tok * top_k // n_exp + 7) // 8) * 8)


def row_sizes(rows):
    return [size for size in (128, 256) if size < rows] + [rows]


def pick_rows(n_rows, rows, body):
    low = 0
    for size in row_sizes(rows):
        high = size if size < rows else rows + 1
        pl.when((n_rows > low if low else n_rows >= 0) & (n_rows <= high))(functools.partial(body, size))
        low = size


def column_pieces(width, step):
    pieces, start = [], 0
    while start < width:
        size = min(step, width - start)
        pieces.append((start, size))
        start += size
    return pieces


def prep_kernel(facts_ref, gates_in_ref, pick_ref, gates_ref):
    top_k = gates_in_ref.shape[2]
    n_tok = pick_ref.shape[2]
    step_rows = 32

    def fill(block, carry):
        at = pl.multiple_of(block * step_rows, step_rows)
        row = lax.broadcasted_iota(jnp.int32, (step_rows, n_tok), 0) + at
        chosen = jnp.zeros((step_rows, n_tok), jnp.float32)
        for j in range(top_k):
            chosen = jnp.where(facts_ref[0, j : j + 1, :] == row, 1.0, chosen)
        pick_ref[0, pl.ds(at, step_rows), :] = chosen.astype(jnp.bfloat16)
        return carry

    lax.fori_loop(0, pick_ref.shape[1] // step_rows, fill, 0)

    def tile(index, carry):
        row = lax.broadcasted_iota(jnp.int32, (256, n_tok), 0) + index * 256
        for piece in range(3):
            weight = jnp.zeros((256, n_tok), jnp.float32)
            for j in range(top_k):
                weight = jnp.where(facts_ref[0, 8 + j : 9 + j, :] == row, gates_in_ref[piece, 0, j : j + 1, :], weight)
            gates_ref[index, piece] = weight.astype(jnp.bfloat16).T
        return carry

    lax.fori_loop(0, gates_ref.shape[0], tile, 0)


def up_kernel(cap, off_ref, n_ref, at1_ref, at2_ref, pick_ref, x0_ref, x1_ref, x2_ref, x3_ref, w1_hbm, w3_hbm, h0_ref, h1_ref, h2_ref, rows_ref, w1_ring, w3_ring, sems):
    step = pl.program_id(0)
    n_steps = pl.num_programs(0)
    d_model = x0_ref.shape[1]
    d_ff = w1_ring.shape[2]
    n_slots = w1_ring.shape[0]
    x_refs = (x0_ref, x1_ref, x2_ref, x3_ref)
    h_refs = (h0_ref, h1_ref, h2_ref)

    def fetch(expert):
        slot = expert % n_slots
        return (
            pltpu.make_async_copy(w1_hbm.at[expert], w1_ring.at[slot], sems.at[0, slot]),
            pltpu.make_async_copy(w3_hbm.at[expert], w3_ring.at[slot], sems.at[1, slot]),
        )

    def start(expert):
        for copy in fetch(expert):
            copy.start()

    @pl.when(step == 0)
    def _():
        for expert in range(n_slots - 1):
            start(expert)

    @pl.when(step + n_slots - 1 < n_steps)
    def _():
        start(step + n_slots - 1)

    @pl.when(step % GROUP == 0)
    def _():
        for src, x_ref in enumerate(x_refs):
            chosen = pick_ref[src]
            for begin, size in column_pieces(d_model, 512):
                got = jnp.dot(chosen, x_ref[:, begin : begin + size], preferred_element_type=jnp.float32).astype(jnp.bfloat16)
                for part in range(GROUP):
                    at = pl.multiple_of(off_ref[(step + part) * 4 + src], 16)
                    rows_ref[part, pl.ds(at, cap), begin : begin + size] = got[part * cap : (part + 1) * cap]

    part = step % GROUP
    slot = step % n_slots
    for copy in fetch(step):
        copy.wait()

    def body(size):
        x = rows_ref[part, :size, :]

        def put(value, begin, width):
            for piece in range(size // ROW_PIECE):
                h_refs[piece][0, :, begin : begin + width] = value[piece * ROW_PIECE : (piece + 1) * ROW_PIECE]

        full = d_ff // 256 * 256
        for begin, width in column_pieces(full, 512):
            gate = jnp.dot(x, w1_ring[slot, :, begin : begin + width], preferred_element_type=jnp.float32)
            up = jnp.dot(x, w3_ring[slot, :, begin : begin + width], preferred_element_type=jnp.float32)
            put((jax.nn.silu(gate) * up).astype(jnp.bfloat16), begin, width)
        if full < d_ff:
            tail = d_ff - full
            both = jnp.concatenate([w1_ring[slot, :, full:], w3_ring[slot, :, full:]], axis=1)
            pair = jnp.dot(x, both, preferred_element_type=jnp.float32)
            put((jax.nn.silu(pair[:, :tail]) * pair[:, tail:]).astype(jnp.bfloat16), full, tail)

    pick_rows(n_ref[step], rows_ref.shape[1], body)


def down_kernel(cap, first, off_ref, n_ref, queue_off_ref, total_ref, h0_hbm, h1_hbm, h2_hbm, w2_hbm, gates_hbm, own_ref, sib_ref, out_ref, queue_ref, w2_ring, h_ring, gates_ref, w_sems, h_sems, gate_sems):
    step = pl.program_id(0)
    n_local = pl.num_programs(0)
    n_slots, _, width_all = w2_ring.shape
    n_tiles_max = gates_ref.shape[0] // 4
    h_hbm = (h0_hbm, h1_hbm, h2_hbm)

    def fetch(expert, act):
        slot = expert % n_slots
        for piece, source in enumerate(h_hbm):
            into = h_ring.at[slot, piece * ROW_PIECE : (piece + 1) * ROW_PIECE]
            copy = pltpu.make_async_copy(source.at[expert], into, h_sems.at[piece, slot])
            pl.when(n_ref[expert] > piece * ROW_PIECE)(functools.partial(act, copy))
        act(pltpu.make_async_copy(w2_hbm.at[expert, :, first : first + width_all], w2_ring.at[slot], w_sems.at[slot]))

    def gate_copies(act):
        for src in range(4):
            for tile in range(n_tiles_max):
                index = src * n_tiles_max + tile
                copy = pltpu.make_async_copy(gates_hbm.at[index], gates_ref.at[index], gate_sems.at[index])
                pl.when(tile * 256 < total_ref[src])(functools.partial(act, copy))

    @pl.when(step == 0)
    def _():
        for expert in range(n_slots - 1):
            fetch(expert, lambda copy: copy.start())

    @pl.when(step + n_slots - 1 < n_local)
    def _():
        fetch(step + n_slots - 1, lambda copy: copy.start())

    @pl.when(step == 0)
    def _():
        gate_copies(lambda copy: copy.start())

    fetch(step, lambda copy: copy.wait())
    slot = step % n_slots

    def body(size):
        h = h_ring[slot, :size, :]
        for begin, width in column_pieces(width_all, 512):
            out = jnp.dot(h, w2_ring[slot, :, begin : begin + width], preferred_element_type=jnp.float32)
            out_ref[:size, begin : begin + width] = out.astype(jnp.bfloat16)

    pick_rows(n_ref[step], out_ref.shape[0], body)
    for src in range(4):
        at = pl.multiple_of(off_ref[step * 4 + src], 16)
        to = pl.multiple_of(queue_off_ref[src * n_local + step], 16)
        queue_ref[src, pl.ds(to, cap), :] = out_ref[pl.ds(at, cap), :]

    @pl.when(step == n_local - 1)
    def _():
        gate_copies(lambda copy: copy.wait())
        for src in range(4):
            total = total_ref[src]
            n_tiles = (total + 255) // 256

            def clear(piece, carry):
                at = pl.multiple_of(total + piece * 16, 16)
                queue_ref[src, pl.ds(at, 16), :] = jnp.zeros((16, width_all), jnp.bfloat16)
                return carry

            lax.fori_loop(0, (n_tiles * 256 - total) // 16, clear, 0)
            into = (own_ref, sib_ref, own_ref, sib_ref)[src]
            place = src // 2
            into[place] = jnp.zeros(into.shape[1:], jnp.float32)

            def add(tile, carry):
                at = pl.multiple_of(tile * 256, 256)
                for begin, width in column_pieces(width_all, 512):
                    held = queue_ref[src, pl.ds(at, 256), begin : begin + width]
                    new = into[place, :, begin : begin + width]
                    for piece in range(3):
                        new += jnp.dot(gates_ref[src * n_tiles_max + tile, piece], held, preferred_element_type=jnp.float32)
                    into[place, :, begin : begin + width] = new
                return carry

            lax.fori_loop(0, n_tiles, add, 0)


def solution(mesh):
    ep_size = mesh.shape["ep"]
    row_spec = P(("data", "ep", "tp"), None)
    expert_spec = P("ep", None, None)
    n_rep = mesh.shape["data"] * ep_size

    def layer_body(tokens, expert_ids, gate_vals, slot_ids, send_counts, shared_w1, shared_w3, shared_w2, expert_w1, expert_w3, expert_w2):
        n_tok, d_model = tokens.shape
        top_k = expert_ids.shape[1]
        n_local, _, d_ff = expert_w1.shape
        n_exp = n_local * ep_size
        cap = capacity_rows(n_tok, top_k, n_exp)
        rows = ep_size * cap
        n_queue = n_local * cap
        me = lax.axis_index("ep")

        def swap(value, bit):
            return lax.ppermute(value, "ep", [(i, i ^ bit) for i in range(ep_size)])

        x_far = swap(tokens, 2)
        x_sib = swap(tokens, 1)
        x_far_sib = swap(x_far, 1)
        all_ids = jnp.arange(n_exp, dtype=jnp.int32)
        row_limit = jnp.sum(jnp.where(expert_ids[:, :, None] == all_ids, send_counts[0], 0), axis=-1)
        kept_mask = (slot_ids >= 0) & (slot_ids < row_limit)
        dest_row = jnp.where(kept_mask, expert_ids * cap + slot_ids, -1)
        facts = jnp.concatenate(
            [
                dest_row.astype(jnp.float32).T,
                jnp.where(kept_mask, gate_vals, 0.0).T,
                jnp.pad(send_counts.astype(jnp.float32), ((0, 0), (0, n_tok - n_exp))),
                jnp.zeros((15 - 2 * top_k, n_tok), jnp.float32),
            ],
            axis=0,
        )
        facts_far = swap(facts, 2)
        facts_sib = swap(facts, 1)
        facts_all = jnp.stack([facts, facts_sib, facts_far, swap(facts_far, 1)])

        dest_all = facts_all[:, :top_k].astype(jnp.int32) - me * n_queue
        dest_all = jnp.where((dest_all >= 0) & (dest_all < n_queue), dest_all, -1)
        gates_all = facts_all[:, top_k : 2 * top_k]
        counts_all = lax.dynamic_slice_in_dim(facts_all[:, 2 * top_k], me * n_local, n_local, 1).astype(jnp.int32)
        padded = (counts_all + 15) // 16 * 16
        local = jnp.arange(n_local, dtype=jnp.int32)
        before = local[None, :] < local[:, None]
        queue_off = jnp.sum(jnp.where(before[None], padded[:, None, :], 0), axis=2)
        total = jnp.sum(padded, axis=1)
        src = jnp.arange(4, dtype=jnp.int32)
        off = jnp.sum(jnp.where((src[None, :] < src[:, None])[None], padded.T[:, None, :], 0), axis=2).reshape(-1)
        n_rows = jnp.sum(padded, axis=0)

        def piece_home(piece):
            need = n_rows > piece * ROW_PIECE
            last = jnp.max(jnp.where(need[None, :] & (local[None, :] <= local[:, None]), local[None, :], -1), axis=1)
            first = jnp.min(jnp.where(need, local, n_local))
            return jnp.where(last >= 0, last, jnp.where(first < n_local, first, 0))

        at1, at2 = piece_home(1), piece_home(2)
        shift = jnp.sum(jnp.where((dest_all // cap)[..., None] == local, (queue_off - local * cap)[:, None, None, :], 0), axis=-1)
        queue_row = jnp.where(dest_all >= 0, dest_all + shift, -1)
        pad_rows = jnp.full((4, 8 - top_k, n_tok), -1, jnp.int32)
        places = jnp.concatenate([dest_all, pad_rows, queue_row, pad_rows], axis=1)
        high = lax.reduce_precision(gates_all, 8, 7)
        middle = lax.reduce_precision(gates_all - high, 8, 7)
        low = lax.reduce_precision(gates_all - high - middle, 8, 7)
        n_tiles = n_queue // 256
        pick, gate_tiles = pl.pallas_call(
            prep_kernel,
            grid=(4,),
            in_specs=[
                pl.BlockSpec((1, 16, n_tok), lambda s: (s, 0, 0)),
                pl.BlockSpec((3, 1, top_k, n_tok), lambda s: (0, s, 0, 0)),
            ],
            out_specs=[
                pl.BlockSpec((1, n_queue, n_tok), lambda s: (s, 0, 0)),
                pl.BlockSpec((n_tiles, 3, n_tok, 256), lambda s: (s, 0, 0, 0)),
            ],
            out_shape=[
                jax.ShapeDtypeStruct((4, n_queue, n_tok), jnp.bfloat16),
                jax.ShapeDtypeStruct((4 * n_tiles, 3, n_tok, 256), jnp.bfloat16),
            ],
            compiler_params=pltpu.CompilerParams(dimension_semantics=("arbitrary",), vmem_limit_bytes=40_000_000),
            cost_estimate=pl.CostEstimate(flops=10**9, bytes_accessed=4 * n_queue * n_tok * 8, transcendentals=0),
            name="prep",
        )(places, jnp.stack([high, middle, low]))

        whole = dict(pipeline_mode=pl.Buffered(1))
        any_space = pl.BlockSpec(memory_space=pl.ANY)
        hidden = pl.pallas_call(
            functools.partial(up_kernel, cap),
            grid_spec=pltpu.PrefetchScalarGridSpec(
                num_scalar_prefetch=4,
                grid=(n_local,),
                in_specs=[
                    pl.BlockSpec((4, GROUP * cap, n_tok), lambda e, *_: (0, e // GROUP, 0)),
                    *[pl.BlockSpec((n_tok, d_model), lambda e, *_: (0, 0), **whole) for _ in range(4)],
                    any_space,
                    any_space,
                ],
                out_specs=[
                    pl.BlockSpec((1, ROW_PIECE, d_ff), lambda e, off, n, at1, at2: (e, 0, 0)),
                    pl.BlockSpec((1, ROW_PIECE, d_ff), lambda e, off, n, at1, at2: (at1[e], 0, 0)),
                    pl.BlockSpec((1, ROW_PIECE, d_ff), lambda e, off, n, at1, at2: (at2[e], 0, 0)),
                ],
                scratch_shapes=[
                    pltpu.VMEM((GROUP, rows, d_model), jnp.bfloat16),
                    pltpu.VMEM((UP_SLOTS, d_model, d_ff), jnp.bfloat16),
                    pltpu.VMEM((UP_SLOTS, d_model, d_ff), jnp.bfloat16),
                    pltpu.SemaphoreType.DMA((2, UP_SLOTS)),
                ],
            ),
            out_shape=[jax.ShapeDtypeStruct((n_local, ROW_PIECE, d_ff), jnp.bfloat16)] * 3,
            compiler_params=pltpu.CompilerParams(dimension_semantics=("arbitrary",), vmem_limit_bytes=VMEM_LIMIT),
            cost_estimate=pl.CostEstimate(flops=4 * n_local * 192 * d_model * d_ff, bytes_accessed=4 * n_local * d_model * d_ff, transcendentals=0),
            name="experts_up",
        )(off, n_rows, at1, at2, pick, tokens, x_sib, x_far, x_far_sib, expert_w1, expert_w3)

        n_cols = d_model // COLUMN_CHUNKS

        def down(chunk, held):
            return pl.pallas_call(
                functools.partial(down_kernel, cap, chunk * n_cols),
                grid_spec=pltpu.PrefetchScalarGridSpec(
                    num_scalar_prefetch=4,
                    grid=(n_local,),
                    in_specs=[any_space] * 5,
                    out_specs=[pl.BlockSpec((2, n_tok, n_cols), lambda e, *_: (0, 0, 0), **whole) for _ in range(2)],
                    scratch_shapes=[
                        pltpu.VMEM((rows, n_cols), jnp.bfloat16),
                        pltpu.VMEM((4, n_queue, n_cols), jnp.bfloat16),
                        pltpu.VMEM((DOWN_SLOTS, d_ff, n_cols), jnp.bfloat16),
                        pltpu.VMEM((DOWN_SLOTS, rows, d_ff), jnp.bfloat16),
                        pltpu.VMEM(gate_tiles.shape, jnp.bfloat16),
                        pltpu.SemaphoreType.DMA((DOWN_SLOTS,)),
                        pltpu.SemaphoreType.DMA((3, DOWN_SLOTS)),
                        pltpu.SemaphoreType.DMA((4 * n_tiles,)),
                    ],
                ),
                out_shape=[jax.ShapeDtypeStruct((2, n_tok, n_cols), jnp.float32) for _ in range(2)],
                compiler_params=pltpu.CompilerParams(dimension_semantics=("arbitrary",), vmem_limit_bytes=VMEM_LIMIT),
                cost_estimate=pl.CostEstimate(flops=2 * n_local * 192 * n_cols * d_ff, bytes_accessed=2 * n_local * n_cols * d_ff, transcendentals=0),
            )(off, n_rows, queue_off.reshape(-1), total, *held, expert_w2, gate_tiles)

        gathered = lax.all_gather(tokens, "tp", axis=0, tiled=True)
        sums_own, sums_sib, returned = [], [], []
        for chunk in range(COLUMN_CHUNKS):
            own, sib = down(chunk, hidden)
            from_sib = swap(sib, 1)
            if chunk == 0:
                gathered, own = lax.optimization_barrier((gathered, own))
                pre_gate = jnp.dot(gathered, shared_w1, preferred_element_type=jnp.float32)
                pre_up = jnp.dot(gathered, shared_w3, preferred_element_type=jnp.float32)
                shared_hidden = (jax.nn.silu(pre_gate) * pre_up).astype(jnp.bfloat16)
            passed_on = own[1] + from_sib[1]
            passed_on, shared_hidden, *hidden = lax.optimization_barrier((passed_on, shared_hidden, *hidden))
            returned.append(swap(passed_on, 2))
            if chunk == 0:
                hidden_blocks = lax.all_to_all(shared_hidden.reshape(mesh.shape["tp"], n_tok, -1), "tp", 0, 0)
            sums_own.append(own[0])
            sums_sib.append(from_sib[0])

        width = shared_w2.shape[0]
        rep = lax.axis_index("data") * ep_size + me
        w2_part = lax.dynamic_slice_in_dim(shared_w2, rep * (width // n_rep), width // n_rep, 0)
        w2_all = lax.all_gather(w2_part, ("tp", "data", "ep"), axis=0, tiled=True)
        w2_all, passed_on = lax.optimization_barrier((w2_all, passed_on))
        w2_blocks = w2_all.reshape(mesh.shape["tp"], width, d_model)
        shared_out = jnp.dot(hidden_blocks[0], w2_blocks[0], preferred_element_type=jnp.float32)
        for block in range(1, mesh.shape["tp"]):
            shared_out += jnp.dot(hidden_blocks[block], w2_blocks[block], preferred_element_type=jnp.float32)
        base = tokens.astype(jnp.float32) + shared_out
        parts = []
        for chunk in range(COLUMN_CHUNKS):
            routed = sums_own[chunk] + sums_sib[chunk] + returned[chunk]
            parts.append((base[:, chunk * n_cols : (chunk + 1) * n_cols] + routed).astype(jnp.bfloat16))
        return jnp.concatenate(parts, axis=1)


    return jax.shard_map(
        layer_body,
        mesh=mesh,
        in_specs=(row_spec, row_spec, row_spec, row_spec, row_spec, P(None, "tp"), P(None, "tp"), P("tp", None), expert_spec, expert_spec, expert_spec),
        out_specs=row_spec,
        check_vma=False,
    )
```

```python
import functools

import jax
import jax.numpy as jnp
from jax import lax
from jax.experimental import pallas as pl
from jax.experimental.pallas import tpu as pltpu
from jax.sharding import PartitionSpec as P


CAP_FACTOR = 4
GROUP = 4
COLUMN_SHARES = (3, 1)
TOKEN_SHARES = (1, 2, 1)
ROW_PIECE = 128
UP_SLOTS = 3
DOWN_SLOTS = 4
VMEM_LIMIT = 66_000_000


def capacity_rows(n_tok, top_k, n_exp):
    return min(n_tok, ((CAP_FACTOR * n_tok * top_k // n_exp + 7) // 8) * 8)


def row_sizes(rows):
    return [size for size in (64, 128, 256) if size < rows] + [rows]


def pick_rows(n_rows, rows, body):
    low = 0
    for size in row_sizes(rows):
        high = size if size < rows else rows + 1
        pl.when((n_rows > low if low else n_rows >= 0) & (n_rows <= high))(functools.partial(body, size))
        low = size


def column_pieces(width, step):
    pieces, start = [], 0
    while start < width:
        size = min(step, width - start)
        pieces.append((start, size))
        start += size
    return pieces


def prep_kernel(facts_ref, gates_in_ref, pick_ref, gates_ref):
    top_k = gates_in_ref.shape[2]
    n_tok = pick_ref.shape[2]
    step_rows = 32

    def fill(block, carry):
        at = pl.multiple_of(block * step_rows, step_rows)
        row = lax.broadcasted_iota(jnp.int32, (step_rows, n_tok), 0) + at
        chosen = jnp.zeros((step_rows, n_tok), jnp.float32)
        for j in range(top_k):
            chosen = jnp.where(facts_ref[0, j : j + 1, :] == row, 1.0, chosen)
        pick_ref[0, pl.ds(at, step_rows), :] = chosen.astype(jnp.bfloat16)
        return carry

    lax.fori_loop(0, pick_ref.shape[1] // step_rows, fill, 0)

    def tile(index, carry):
        row = lax.broadcasted_iota(jnp.int32, (256, n_tok), 0) + index * 256
        for piece in range(3):
            weight = jnp.zeros((256, n_tok), jnp.float32)
            for j in range(top_k):
                weight = jnp.where(facts_ref[0, 8 + j : 9 + j, :] == row, gates_in_ref[piece, 0, j : j + 1, :], weight)
            gates_ref[index, piece] = weight.astype(jnp.bfloat16).T
        return carry

    lax.fori_loop(0, gates_ref.shape[0], tile, 0)


def up_kernel(cap, off_ref, n_ref, at1_ref, at2_ref, pick_ref, x0_ref, x1_ref, x2a_ref, x2b_ref, x2c_ref, x3a_ref, x3b_ref, x3c_ref, w1_hbm, w3_hbm, h0_ref, h1_ref, h2_ref, rows_ref, w1_ring, w3_ring, sems):
    step = pl.program_id(0)
    n_steps = pl.num_programs(0)
    d_model = x0_ref.shape[1]
    d_ff = w1_ring.shape[2]
    n_slots = w1_ring.shape[0]
    x_refs = ((x0_ref,), (x1_ref,), (x2a_ref, x2b_ref, x2c_ref), (x3a_ref, x3b_ref, x3c_ref))
    piece_step = min(512, d_model // sum(TOKEN_SHARES))
    h_refs = (h0_ref, h1_ref, h2_ref)

    def fetch(expert):
        slot = expert % n_slots
        return (
            pltpu.make_async_copy(w1_hbm.at[expert], w1_ring.at[slot], sems.at[0, slot]),
            pltpu.make_async_copy(w3_hbm.at[expert], w3_ring.at[slot], sems.at[1, slot]),
        )

    def start(expert):
        for copy in fetch(expert):
            copy.start()

    @pl.when(step == 0)
    def _():
        for expert in range(n_slots - 1):
            start(expert)

    @pl.when(step + n_slots - 1 < n_steps)
    def _():
        start(step + n_slots - 1)

    @pl.when(step % GROUP == 0)
    def _():
        for src, pieces in enumerate(x_refs):
            chosen = pick_ref[src]
            base = 0
            for x_ref in pieces:
                for begin, size in column_pieces(x_ref.shape[1], piece_step):
                    got = jnp.dot(chosen, x_ref[:, begin : begin + size], preferred_element_type=jnp.float32).astype(jnp.bfloat16)
                    for part in range(GROUP):
                        at = pl.multiple_of(off_ref[(step + part) * 4 + src], 16)
                        rows_ref[part, pl.ds(at, cap), base + begin : base + begin + size] = got[part * cap : (part + 1) * cap]
                base += x_ref.shape[1]

    part = step % GROUP
    slot = step % n_slots
    for copy in fetch(step):
        copy.wait()

    def body(size):
        x = rows_ref[part, :size, :]

        def put(value, begin, width):
            for piece in range(-(-size // ROW_PIECE)):
                part_rows = min(size - piece * ROW_PIECE, ROW_PIECE)
                h_refs[piece][0, :part_rows, begin : begin + width] = value[piece * ROW_PIECE : piece * ROW_PIECE + part_rows]

        full = d_ff // 256 * 256
        for begin, width in column_pieces(full, 512):
            gate = jnp.dot(x, w1_ring[slot, :, begin : begin + width], preferred_element_type=jnp.float32)
            up = jnp.dot(x, w3_ring[slot, :, begin : begin + width], preferred_element_type=jnp.float32)
            put((jax.nn.silu(gate) * up).astype(jnp.bfloat16), begin, width)
        if full < d_ff:
            tail = d_ff - full
            both = jnp.concatenate([w1_ring[slot, :, full:], w3_ring[slot, :, full:]], axis=1)
            pair = jnp.dot(x, both, preferred_element_type=jnp.float32)
            put((jax.nn.silu(pair[:, :tail]) * pair[:, tail:]).astype(jnp.bfloat16), full, tail)

    pick_rows(n_ref[step], rows_ref.shape[1], body)


def down_kernel(cap, first, off_ref, n_ref, queue_off_ref, total_ref, h0_hbm, h1_hbm, h2_hbm, w2_hbm, gates_hbm, own_ref, sib_ref, out_ref, queue_ref, w2_ring, h_ring, gates_ref, w_sems, h_sems, gate_sems):
    step = pl.program_id(0)
    n_local = pl.num_programs(0)
    n_slots, _, width_all = w2_ring.shape
    n_tiles_max = gates_ref.shape[0] // 4
    h_hbm = (h0_hbm, h1_hbm, h2_hbm)

    def fetch(expert, act):
        slot = expert % n_slots
        for piece, source in enumerate(h_hbm):
            into = h_ring.at[slot, piece * ROW_PIECE : (piece + 1) * ROW_PIECE]
            copy = pltpu.make_async_copy(source.at[expert], into, h_sems.at[piece, slot])
            pl.when(n_ref[expert] > piece * ROW_PIECE)(functools.partial(act, copy))
        act(pltpu.make_async_copy(w2_hbm.at[expert, :, first : first + width_all], w2_ring.at[slot], w_sems.at[slot]))

    def gate_copies(act):
        for src in range(4):
            for tile in range(n_tiles_max):
                index = src * n_tiles_max + tile
                copy = pltpu.make_async_copy(gates_hbm.at[index], gates_ref.at[index], gate_sems.at[index])
                pl.when(tile * 256 < total_ref[src])(functools.partial(act, copy))

    @pl.when(step == 0)
    def _():
        for expert in range(n_slots - 1):
            fetch(expert, lambda copy: copy.start())

    @pl.when(step + n_slots - 1 < n_local)
    def _():
        fetch(step + n_slots - 1, lambda copy: copy.start())

    @pl.when(step == 0)
    def _():
        gate_copies(lambda copy: copy.start())

    fetch(step, lambda copy: copy.wait())
    slot = step % n_slots

    def body(size):
        h = h_ring[slot, :size, :]
        for begin, width in column_pieces(width_all, 512):
            out = jnp.dot(h, w2_ring[slot, :, begin : begin + width], preferred_element_type=jnp.float32)
            out_ref[:size, begin : begin + width] = out.astype(jnp.bfloat16)

    pick_rows(n_ref[step], out_ref.shape[0], body)
    for src in range(4):
        at = pl.multiple_of(off_ref[step * 4 + src], 16)
        to = pl.multiple_of(queue_off_ref[src * n_local + step], 16)
        end = off_ref[step * 4 + src + 1] if src < 3 else n_ref[step]

        def keep(size, at=at, to=to, src=src):
            queue_ref[src, pl.ds(to, size), :] = out_ref[pl.ds(at, size), :]

        few = min(32, cap)
        pl.when(end - at <= few)(functools.partial(keep, few))
        pl.when(end - at > few)(functools.partial(keep, cap))

    @pl.when(step == n_local - 1)
    def _():
        gate_copies(lambda copy: copy.wait())
        for src in range(4):
            total = total_ref[src]
            n_tiles = (total + 255) // 256

            def clear(piece, carry):
                at = pl.multiple_of(total + piece * 16, 16)
                queue_ref[src, pl.ds(at, 16), :] = jnp.zeros((16, width_all), jnp.bfloat16)
                return carry

            lax.fori_loop(0, (n_tiles * 256 - total) // 16, clear, 0)
            into = (own_ref, sib_ref, own_ref, sib_ref)[src]
            place = src // 2
            into[place] = jnp.zeros(into.shape[1:], jnp.float32)

            def add(tile, carry):
                at = pl.multiple_of(tile * 256, 256)
                for begin, width in column_pieces(width_all, 512):
                    held = queue_ref[src, pl.ds(at, 256), begin : begin + width]
                    new = into[place, :, begin : begin + width]
                    for piece in range(3):
                        new += jnp.dot(gates_ref[src * n_tiles_max + tile, piece], held, preferred_element_type=jnp.float32)
                    into[place, :, begin : begin + width] = new
                return carry

            lax.fori_loop(0, n_tiles, add, 0)


def solution(mesh):
    ep_size = mesh.shape["ep"]
    row_spec = P(("data", "ep", "tp"), None)
    expert_spec = P("ep", None, None)
    n_rep = mesh.shape["data"] * ep_size

    def layer_body(tokens, expert_ids, gate_vals, slot_ids, send_counts, shared_w1, shared_w3, shared_w2, expert_w1, expert_w3, expert_w2):
        n_tok, d_model = tokens.shape
        top_k = expert_ids.shape[1]
        n_local, _, d_ff = expert_w1.shape
        n_exp = n_local * ep_size
        cap = capacity_rows(n_tok, top_k, n_exp)
        rows = ep_size * cap
        n_queue = n_local * cap
        me = lax.axis_index("ep")

        def swap(value, bit):
            return lax.ppermute(value, "ep", [(i, i ^ bit) for i in range(ep_size)])

        x_far, x_far_sib, begin = [], [], 0
        for share in TOKEN_SHARES:
            size = d_model * share // sum(TOKEN_SHARES)
            x_far.append(swap(tokens[:, begin : begin + size], 2))
            x_far_sib.append(swap(x_far[-1], 1))
            begin += size
        x_sib = swap(tokens, 1)
        all_ids = jnp.arange(n_exp, dtype=jnp.int32)
        row_limit = jnp.sum(jnp.where(expert_ids[:, :, None] == all_ids, send_counts[0], 0), axis=-1)
        kept_mask = (slot_ids >= 0) & (slot_ids < row_limit)
        dest_row = jnp.where(kept_mask, expert_ids * cap + slot_ids, -1)
        facts = jnp.concatenate(
            [
                dest_row.astype(jnp.float32).T,
                jnp.where(kept_mask, gate_vals, 0.0).T,
                jnp.pad(send_counts.astype(jnp.float32), ((0, 0), (0, n_tok - n_exp))),
                jnp.zeros((15 - 2 * top_k, n_tok), jnp.float32),
            ],
            axis=0,
        )
        facts_far = swap(facts, 2)
        facts_sib = swap(facts, 1)
        facts_all = jnp.stack([facts, facts_sib, facts_far, swap(facts_far, 1)])

        dest_all = facts_all[:, :top_k].astype(jnp.int32) - me * n_queue
        dest_all = jnp.where((dest_all >= 0) & (dest_all < n_queue), dest_all, -1)
        gates_all = facts_all[:, top_k : 2 * top_k]
        counts_all = lax.dynamic_slice_in_dim(facts_all[:, 2 * top_k], me * n_local, n_local, 1).astype(jnp.int32)
        padded = (counts_all + 15) // 16 * 16
        local = jnp.arange(n_local, dtype=jnp.int32)
        before = local[None, :] < local[:, None]
        queue_off = jnp.sum(jnp.where(before[None], padded[:, None, :], 0), axis=2)
        total = jnp.sum(padded, axis=1)
        src = jnp.arange(4, dtype=jnp.int32)
        off = jnp.sum(jnp.where((src[None, :] < src[:, None])[None], padded.T[:, None, :], 0), axis=2).reshape(-1)
        n_rows = jnp.sum(padded, axis=0)

        def piece_home(piece):
            need = n_rows > piece * ROW_PIECE
            last = jnp.max(jnp.where(need[None, :] & (local[None, :] <= local[:, None]), local[None, :], -1), axis=1)
            first = jnp.min(jnp.where(need, local, n_local))
            return jnp.where(last >= 0, last, jnp.where(first < n_local, first, 0))

        at1, at2 = piece_home(1), piece_home(2)
        shift = jnp.sum(jnp.where((dest_all // cap)[..., None] == local, (queue_off - local * cap)[:, None, None, :], 0), axis=-1)
        queue_row = jnp.where(dest_all >= 0, dest_all + shift, -1)
        pad_rows = jnp.full((4, 8 - top_k, n_tok), -1, jnp.int32)
        places = jnp.concatenate([dest_all, pad_rows, queue_row, pad_rows], axis=1)
        high = lax.reduce_precision(gates_all, 8, 7)
        middle = lax.reduce_precision(gates_all - high, 8, 7)
        low = lax.reduce_precision(gates_all - high - middle, 8, 7)
        n_tiles = n_queue // 256
        pick, gate_tiles = pl.pallas_call(
            prep_kernel,
            grid=(4,),
            in_specs=[
                pl.BlockSpec((1, 16, n_tok), lambda s: (s, 0, 0)),
                pl.BlockSpec((3, 1, top_k, n_tok), lambda s: (0, s, 0, 0)),
            ],
            out_specs=[
                pl.BlockSpec((1, n_queue, n_tok), lambda s: (s, 0, 0)),
                pl.BlockSpec((n_tiles, 3, n_tok, 256), lambda s: (s, 0, 0, 0)),
            ],
            out_shape=[
                pltpu.HBM((4, n_queue, n_tok), jnp.bfloat16),
                pltpu.HBM((4 * n_tiles, 3, n_tok, 256), jnp.bfloat16),
            ],
            compiler_params=pltpu.CompilerParams(dimension_semantics=("arbitrary",), vmem_limit_bytes=40_000_000),
            cost_estimate=pl.CostEstimate(flops=10**9, bytes_accessed=4 * n_queue * n_tok * 8, transcendentals=0),
            name="prep",
        )(places, jnp.stack([high, middle, low]))

        whole = dict(pipeline_mode=pl.Buffered(1))
        any_space = pl.BlockSpec(memory_space=pl.ANY)
        hidden = pl.pallas_call(
            functools.partial(up_kernel, cap),
            grid_spec=pltpu.PrefetchScalarGridSpec(
                num_scalar_prefetch=4,
                grid=(n_local,),
                in_specs=[
                    pl.BlockSpec((4, GROUP * cap, n_tok), lambda e, *_: (0, e // GROUP, 0)),
                    *[pl.BlockSpec(x.shape, lambda e, *_: (0, 0), **whole) for x in (tokens, x_sib, *x_far, *x_far_sib)],
                    any_space,
                    any_space,
                ],
                out_specs=[
                    pl.BlockSpec((1, ROW_PIECE, d_ff), lambda e, off, n, at1, at2: (e, 0, 0)),
                    pl.BlockSpec((1, ROW_PIECE, d_ff), lambda e, off, n, at1, at2: (at1[e], 0, 0)),
                    pl.BlockSpec((1, ROW_PIECE, d_ff), lambda e, off, n, at1, at2: (at2[e], 0, 0)),
                ],
                scratch_shapes=[
                    pltpu.VMEM((GROUP, rows, d_model), jnp.bfloat16),
                    pltpu.VMEM((UP_SLOTS, d_model, d_ff), jnp.bfloat16),
                    pltpu.VMEM((UP_SLOTS, d_model, d_ff), jnp.bfloat16),
                    pltpu.SemaphoreType.DMA((2, UP_SLOTS)),
                ],
            ),
            out_shape=[jax.ShapeDtypeStruct((n_local, ROW_PIECE, d_ff), jnp.bfloat16)] * 3,
            compiler_params=pltpu.CompilerParams(dimension_semantics=("arbitrary",), vmem_limit_bytes=VMEM_LIMIT),
            cost_estimate=pl.CostEstimate(flops=4 * n_local * 192 * d_model * d_ff, bytes_accessed=4 * n_local * d_model * d_ff, transcendentals=0),
            name="experts_up",
        )(off, n_rows, at1, at2, pick, tokens, x_sib, *x_far, *x_far_sib, expert_w1, expert_w3)

        widths = [d_model * share // sum(COLUMN_SHARES) for share in COLUMN_SHARES]
        starts = [sum(widths[:chunk]) for chunk in range(len(widths))]

        def down(chunk, held):
            n_cols = widths[chunk]
            slots = 3 if n_cols > d_model // 2 else DOWN_SLOTS
            return pl.pallas_call(
                functools.partial(down_kernel, cap, starts[chunk]),
                grid_spec=pltpu.PrefetchScalarGridSpec(
                    num_scalar_prefetch=4,
                    grid=(n_local,),
                    in_specs=[any_space] * 5,
                    out_specs=[pl.BlockSpec((2, n_tok, n_cols), lambda e, *_: (0, 0, 0), **whole) for _ in range(2)],
                    scratch_shapes=[
                        pltpu.VMEM((rows, n_cols), jnp.bfloat16),
                        pltpu.VMEM((4, n_queue, n_cols), jnp.bfloat16),
                        pltpu.VMEM((slots, d_ff, n_cols), jnp.bfloat16),
                        pltpu.VMEM((slots, rows, d_ff), jnp.bfloat16),
                        pltpu.VMEM(gate_tiles.shape, jnp.bfloat16),
                        pltpu.SemaphoreType.DMA((slots,)),
                        pltpu.SemaphoreType.DMA((3, slots)),
                        pltpu.SemaphoreType.DMA((4 * n_tiles,)),
                    ],
                ),
                out_shape=[jax.ShapeDtypeStruct((2, n_tok, n_cols), jnp.float32) for _ in range(2)],
                compiler_params=pltpu.CompilerParams(dimension_semantics=("arbitrary",), vmem_limit_bytes=VMEM_LIMIT),
                cost_estimate=pl.CostEstimate(flops=2 * n_local * 192 * n_cols * d_ff, bytes_accessed=2 * n_local * n_cols * d_ff, transcendentals=0),
            )(off, n_rows, queue_off.reshape(-1), total, *held, expert_w2, gate_tiles)

        gathered = lax.all_gather(tokens, "tp", axis=0, tiled=True)
        sums_own, sums_sib, returned = [], [], []
        for chunk in range(len(widths)):
            own, sib = down(chunk, hidden)
            from_sib = swap(sib, 1)
            passed_on = own[1] + from_sib[1]
            returned.append(swap(passed_on, 2))
            sums_own.append(own[0])
            sums_sib.append(from_sib[0])
            if chunk == 0:
                gathered, passed_on = lax.optimization_barrier((gathered, passed_on))
                pre_gate = jnp.dot(gathered, shared_w1, preferred_element_type=jnp.float32)
                pre_up = jnp.dot(gathered, shared_w3, preferred_element_type=jnp.float32)
                shared_hidden = (jax.nn.silu(pre_gate) * pre_up).astype(jnp.bfloat16)
                shared_hidden, *hidden = lax.optimization_barrier((shared_hidden, *hidden))
                hidden_blocks = lax.all_to_all(shared_hidden.reshape(mesh.shape["tp"], n_tok, -1), "tp", 0, 0)

        width = shared_w2.shape[0]
        rep = lax.axis_index("data") * ep_size + me
        w2_part = lax.dynamic_slice_in_dim(shared_w2, rep * (width // n_rep), width // n_rep, 0)
        w2_all = lax.all_gather(w2_part, ("tp", "data", "ep"), axis=0, tiled=True)
        w2_all, passed_on = lax.optimization_barrier((w2_all, passed_on))
        w2_blocks = w2_all.reshape(mesh.shape["tp"], width, d_model)
        shared_out = jnp.dot(hidden_blocks[0], w2_blocks[0], preferred_element_type=jnp.float32)
        for block in range(1, mesh.shape["tp"]):
            shared_out += jnp.dot(hidden_blocks[block], w2_blocks[block], preferred_element_type=jnp.float32)
        base = tokens.astype(jnp.float32) + shared_out
        parts = []
        for chunk, (first, n_cols) in enumerate(zip(starts, widths)):
            routed = sums_own[chunk] + sums_sib[chunk] + returned[chunk]
            parts.append((base[:, first : first + n_cols] + routed).astype(jnp.bfloat16))
        return jnp.concatenate(parts, axis=1)


    return jax.shard_map(
        layer_body,
        mesh=mesh,
        in_specs=(row_spec, row_spec, row_spec, row_spec, row_spec, P(None, "tp"), P(None, "tp"), P("tp", None), expert_spec, expert_spec, expert_spec),
        out_specs=row_spec,
        check_vma=False,
    )
```

```python
import functools

import jax
import jax.numpy as jnp
from jax import lax
from jax.experimental import pallas as pl
from jax.experimental.pallas import tpu as pltpu
from jax.sharding import PartitionSpec as P


CAP_FACTOR = 4
GROUP = 4
COLUMN_SHARES = (5, 3)
TOKEN_SHARES = (3, 1)
ROW_PIECE = 128
UP_SLOTS = 3
DOWN_SLOTS = 4
VMEM_LIMIT = 66_000_000


def capacity_rows(n_tok, top_k, n_exp):
    return min(n_tok, ((CAP_FACTOR * n_tok * top_k // n_exp + 7) // 8) * 8)


def row_sizes(rows):
    return [size for size in (64, 128, 256) if size < rows] + [rows]


def pick_rows(n_rows, rows, body):
    low = 0
    for size in row_sizes(rows):
        high = size if size < rows else rows + 1
        pl.when((n_rows > low if low else n_rows >= 0) & (n_rows <= high))(functools.partial(body, size))
        low = size


def column_pieces(width, step):
    pieces, start = [], 0
    while start < width:
        size = min(step, width - start)
        pieces.append((start, size))
        start += size
    return pieces


def prep_kernel(facts_ref, gates_in_ref, pick_ref, gates_ref):
    top_k = gates_in_ref.shape[2]
    n_tok = pick_ref.shape[2]
    step_rows = 32

    def fill(block, carry):
        at = pl.multiple_of(block * step_rows, step_rows)
        row = lax.broadcasted_iota(jnp.int32, (step_rows, n_tok), 0) + at
        chosen = jnp.zeros((step_rows, n_tok), jnp.float32)
        for j in range(top_k):
            chosen = jnp.where(facts_ref[0, j : j + 1, :] == row, 1.0, chosen)
        pick_ref[0, pl.ds(at, step_rows), :] = chosen.astype(jnp.bfloat16)
        return carry

    lax.fori_loop(0, pick_ref.shape[1] // step_rows, fill, 0)

    def tile(index, carry):
        row = lax.broadcasted_iota(jnp.int32, (256, n_tok), 0) + index * 256
        for piece in range(3):
            weight = jnp.zeros((256, n_tok), jnp.float32)
            for j in range(top_k):
                weight = jnp.where(facts_ref[0, 8 + j : 9 + j, :] == row, gates_in_ref[piece, 0, j : j + 1, :], weight)
            gates_ref[index, piece] = weight.astype(jnp.bfloat16).T
        return carry

    lax.fori_loop(0, gates_ref.shape[0], tile, 0)


def up_kernel(cap, off_ref, n_ref, at1_ref, at2_ref, pick_ref, x0_ref, x1_ref, x2a_ref, x2b_ref, x3a_ref, x3b_ref, w1_hbm, w3_hbm, h0_ref, h1_ref, h2_ref, rows_ref, w1_ring, w3_ring, sems):
    step = pl.program_id(0)
    n_steps = pl.num_programs(0)
    d_model = x0_ref.shape[1]
    d_ff = w1_ring.shape[2]
    n_slots = w1_ring.shape[0]
    x_refs = ((x0_ref,), (x1_ref,), (x2a_ref, x2b_ref), (x3a_ref, x3b_ref))
    piece_step = min(512, d_model // sum(TOKEN_SHARES))
    h_refs = (h0_ref, h1_ref, h2_ref)

    def fetch(expert):
        slot = expert % n_slots
        return (
            pltpu.make_async_copy(w1_hbm.at[expert], w1_ring.at[slot], sems.at[0, slot]),
            pltpu.make_async_copy(w3_hbm.at[expert], w3_ring.at[slot], sems.at[1, slot]),
        )

    def start(expert):
        for copy in fetch(expert):
            copy.start()

    @pl.when(step == 0)
    def _():
        for expert in range(n_slots - 1):
            start(expert)

    @pl.when(step + n_slots - 1 < n_steps)
    def _():
        start(step + n_slots - 1)

    @pl.when(step % GROUP == 0)
    def _():
        for src, pieces in enumerate(x_refs):
            chosen = pick_ref[src]
            base = 0
            for x_ref in pieces:
                for begin, size in column_pieces(x_ref.shape[1], piece_step):
                    got = jnp.dot(chosen, x_ref[:, begin : begin + size], preferred_element_type=jnp.float32).astype(jnp.bfloat16)
                    for part in range(GROUP):
                        at = pl.multiple_of(off_ref[(step + part) * 4 + src], 16)
                        rows_ref[part, pl.ds(at, cap), base + begin : base + begin + size] = got[part * cap : (part + 1) * cap]
                base += x_ref.shape[1]

    part = step % GROUP
    slot = step % n_slots
    for copy in fetch(step):
        copy.wait()

    def body(size):
        x = rows_ref[part, :size, :]

        def put(value, begin, width):
            for piece in range(-(-size // ROW_PIECE)):
                part_rows = min(size - piece * ROW_PIECE, ROW_PIECE)
                h_refs[piece][0, :part_rows, begin : begin + width] = value[piece * ROW_PIECE : piece * ROW_PIECE + part_rows]

        full = d_ff // 256 * 256
        for begin, width in column_pieces(full, 512):
            gate = jnp.dot(x, w1_ring[slot, :, begin : begin + width], preferred_element_type=jnp.float32)
            up = jnp.dot(x, w3_ring[slot, :, begin : begin + width], preferred_element_type=jnp.float32)
            put((jax.nn.silu(gate) * up).astype(jnp.bfloat16), begin, width)
        if full < d_ff:
            tail = d_ff - full
            both = jnp.concatenate([w1_ring[slot, :, full:], w3_ring[slot, :, full:]], axis=1)
            pair = jnp.dot(x, both, preferred_element_type=jnp.float32)
            put((jax.nn.silu(pair[:, :tail]) * pair[:, tail:]).astype(jnp.bfloat16), full, tail)

    pick_rows(n_ref[step], rows_ref.shape[1], body)


def down_kernel(cap, first, off_ref, n_ref, queue_off_ref, total_ref, h0_hbm, h1_hbm, h2_hbm, w2_hbm, gates_hbm, own_ref, sib_ref, out_ref, queue_ref, w2_ring, h_ring, gates_ref, w_sems, h_sems, gate_sems):
    step = pl.program_id(0)
    n_local = pl.num_programs(0)
    n_slots, _, width_all = w2_ring.shape
    n_tiles_max = gates_ref.shape[0] // 4
    h_hbm = (h0_hbm, h1_hbm, h2_hbm)

    def fetch(expert, act):
        slot = expert % n_slots
        for piece, source in enumerate(h_hbm):
            into = h_ring.at[slot, piece * ROW_PIECE : (piece + 1) * ROW_PIECE]
            copy = pltpu.make_async_copy(source.at[expert], into, h_sems.at[piece, slot])
            pl.when(n_ref[expert] > piece * ROW_PIECE)(functools.partial(act, copy))
        act(pltpu.make_async_copy(w2_hbm.at[expert, :, first : first + width_all], w2_ring.at[slot], w_sems.at[slot]))

    def gate_copies(act):
        for src in range(4):
            for tile in range(n_tiles_max):
                index = src * n_tiles_max + tile
                copy = pltpu.make_async_copy(gates_hbm.at[index], gates_ref.at[index], gate_sems.at[index])
                pl.when(tile * 256 < total_ref[src])(functools.partial(act, copy))

    @pl.when(step == 0)
    def _():
        for expert in range(n_slots - 1):
            fetch(expert, lambda copy: copy.start())

    @pl.when(step + n_slots - 1 < n_local)
    def _():
        fetch(step + n_slots - 1, lambda copy: copy.start())

    @pl.when(step == 0)
    def _():
        gate_copies(lambda copy: copy.start())

    fetch(step, lambda copy: copy.wait())
    slot = step % n_slots

    def body(size):
        h = h_ring[slot, :size, :]
        for begin, width in column_pieces(width_all, 512):
            out = jnp.dot(h, w2_ring[slot, :, begin : begin + width], preferred_element_type=jnp.float32)
            out_ref[:size, begin : begin + width] = out.astype(jnp.bfloat16)

    pick_rows(n_ref[step], out_ref.shape[0], body)
    for src in range(4):
        at = pl.multiple_of(off_ref[step * 4 + src], 16)
        to = pl.multiple_of(queue_off_ref[src * n_local + step], 16)
        end = off_ref[step * 4 + src + 1] if src < 3 else n_ref[step]

        def keep(size, at=at, to=to, src=src):
            queue_ref[src, pl.ds(to, size), :] = out_ref[pl.ds(at, size), :]

        few = min(32, cap)
        pl.when(end - at <= few)(functools.partial(keep, few))
        pl.when(end - at > few)(functools.partial(keep, cap))

    @pl.when(step == n_local - 1)
    def _():
        gate_copies(lambda copy: copy.wait())
        for src in range(4):
            total = total_ref[src]
            n_tiles = (total + 255) // 256

            def clear(piece, carry):
                at = pl.multiple_of(total + piece * 16, 16)
                queue_ref[src, pl.ds(at, 16), :] = jnp.zeros((16, width_all), jnp.bfloat16)
                return carry

            lax.fori_loop(0, (n_tiles * 256 - total) // 16, clear, 0)
            into = (own_ref, sib_ref, own_ref, sib_ref)[src]
            place = src // 2
            into[place] = jnp.zeros(into.shape[1:], jnp.float32)

            def add(tile, carry):
                at = pl.multiple_of(tile * 256, 256)
                for begin, width in column_pieces(width_all, 512):
                    held = queue_ref[src, pl.ds(at, 256), begin : begin + width]
                    new = into[place, :, begin : begin + width]
                    for piece in range(3):
                        new += jnp.dot(gates_ref[src * n_tiles_max + tile, piece], held, preferred_element_type=jnp.float32)
                    into[place, :, begin : begin + width] = new
                return carry

            lax.fori_loop(0, n_tiles, add, 0)


def solution(mesh):
    ep_size = mesh.shape["ep"]
    row_spec = P(("data", "ep", "tp"), None)
    expert_spec = P("ep", None, None)
    n_rep = mesh.shape["data"] * ep_size

    def layer_body(tokens, expert_ids, gate_vals, slot_ids, send_counts, shared_w1, shared_w3, shared_w2, expert_w1, expert_w3, expert_w2):
        n_tok, d_model = tokens.shape
        top_k = expert_ids.shape[1]
        n_local, _, d_ff = expert_w1.shape
        n_exp = n_local * ep_size
        cap = capacity_rows(n_tok, top_k, n_exp)
        rows = ep_size * cap
        n_queue = n_local * cap
        me = lax.axis_index("ep")

        def swap(value, bit):
            return lax.ppermute(value, "ep", [(i, i ^ bit) for i in range(ep_size)])

        x_far, x_far_sib, begin = [], [], 0
        for share in TOKEN_SHARES:
            size = d_model * share // sum(TOKEN_SHARES)
            x_far.append(swap(tokens[:, begin : begin + size], 2))
            x_far_sib.append(swap(x_far[-1], 1))
            begin += size
        x_sib = swap(tokens, 1)
        all_ids = jnp.arange(n_exp, dtype=jnp.int32)
        row_limit = jnp.sum(jnp.where(expert_ids[:, :, None] == all_ids, send_counts[0], 0), axis=-1)
        kept_mask = (slot_ids >= 0) & (slot_ids < row_limit)
        dest_row = jnp.where(kept_mask, expert_ids * cap + slot_ids, -1)
        facts = jnp.concatenate(
            [
                dest_row.astype(jnp.float32).T,
                jnp.where(kept_mask, gate_vals, 0.0).T,
                jnp.pad(send_counts.astype(jnp.float32), ((0, 0), (0, n_tok - n_exp))),
                jnp.zeros((15 - 2 * top_k, n_tok), jnp.float32),
            ],
            axis=0,
        )
        facts_far = swap(facts, 2)
        facts_sib = swap(facts, 1)
        facts_all = jnp.stack([facts, facts_sib, facts_far, swap(facts_far, 1)])

        dest_all = facts_all[:, :top_k].astype(jnp.int32) - me * n_queue
        dest_all = jnp.where((dest_all >= 0) & (dest_all < n_queue), dest_all, -1)
        gates_all = facts_all[:, top_k : 2 * top_k]
        counts_all = lax.dynamic_slice_in_dim(facts_all[:, 2 * top_k], me * n_local, n_local, 1).astype(jnp.int32)
        padded = (counts_all + 15) // 16 * 16
        local = jnp.arange(n_local, dtype=jnp.int32)
        before = local[None, :] < local[:, None]
        queue_off = jnp.sum(jnp.where(before[None], padded[:, None, :], 0), axis=2)
        total = jnp.sum(padded, axis=1)
        src = jnp.arange(4, dtype=jnp.int32)
        off = jnp.sum(jnp.where((src[None, :] < src[:, None])[None], padded.T[:, None, :], 0), axis=2).reshape(-1)
        n_rows = jnp.sum(padded, axis=0)

        def piece_home(piece):
            need = n_rows > piece * ROW_PIECE
            last = jnp.max(jnp.where(need[None, :] & (local[None, :] <= local[:, None]), local[None, :], -1), axis=1)
            first = jnp.min(jnp.where(need, local, n_local))
            return jnp.where(last >= 0, last, jnp.where(first < n_local, first, 0))

        at1, at2 = piece_home(1), piece_home(2)
        shift = jnp.sum(jnp.where((dest_all // cap)[..., None] == local, (queue_off - local * cap)[:, None, None, :], 0), axis=-1)
        queue_row = jnp.where(dest_all >= 0, dest_all + shift, -1)
        pad_rows = jnp.full((4, 8 - top_k, n_tok), -1, jnp.int32)
        places = jnp.concatenate([dest_all, pad_rows, queue_row, pad_rows], axis=1)
        high = lax.reduce_precision(gates_all, 8, 7)
        middle = lax.reduce_precision(gates_all - high, 8, 7)
        low = lax.reduce_precision(gates_all - high - middle, 8, 7)
        n_tiles = n_queue // 256
        pick, gate_tiles = pl.pallas_call(
            prep_kernel,
            grid=(4,),
            in_specs=[
                pl.BlockSpec((1, 16, n_tok), lambda s: (s, 0, 0)),
                pl.BlockSpec((3, 1, top_k, n_tok), lambda s: (0, s, 0, 0)),
            ],
            out_specs=[
                pl.BlockSpec((1, n_queue, n_tok), lambda s: (s, 0, 0)),
                pl.BlockSpec((n_tiles, 3, n_tok, 256), lambda s: (s, 0, 0, 0)),
            ],
            out_shape=[
                pltpu.HBM((4, n_queue, n_tok), jnp.bfloat16),
                pltpu.HBM((4 * n_tiles, 3, n_tok, 256), jnp.bfloat16),
            ],
            compiler_params=pltpu.CompilerParams(dimension_semantics=("arbitrary",), vmem_limit_bytes=40_000_000),
            cost_estimate=pl.CostEstimate(flops=10**9, bytes_accessed=4 * n_queue * n_tok * 8, transcendentals=0),
            name="prep",
        )(places, jnp.stack([high, middle, low]))

        whole = dict(pipeline_mode=pl.Buffered(1))
        any_space = pl.BlockSpec(memory_space=pl.ANY)
        hidden = pl.pallas_call(
            functools.partial(up_kernel, cap),
            grid_spec=pltpu.PrefetchScalarGridSpec(
                num_scalar_prefetch=4,
                grid=(n_local,),
                in_specs=[
                    pl.BlockSpec((4, GROUP * cap, n_tok), lambda e, *_: (0, e // GROUP, 0)),
                    *[pl.BlockSpec(x.shape, lambda e, *_: (0, 0), **whole) for x in (tokens, x_sib, *x_far, *x_far_sib)],
                    any_space,
                    any_space,
                ],
                out_specs=[
                    pl.BlockSpec((1, ROW_PIECE, d_ff), lambda e, off, n, at1, at2: (e, 0, 0)),
                    pl.BlockSpec((1, ROW_PIECE, d_ff), lambda e, off, n, at1, at2: (at1[e], 0, 0)),
                    pl.BlockSpec((1, ROW_PIECE, d_ff), lambda e, off, n, at1, at2: (at2[e], 0, 0)),
                ],
                scratch_shapes=[
                    pltpu.VMEM((GROUP, rows, d_model), jnp.bfloat16),
                    pltpu.VMEM((UP_SLOTS, d_model, d_ff), jnp.bfloat16),
                    pltpu.VMEM((UP_SLOTS, d_model, d_ff), jnp.bfloat16),
                    pltpu.SemaphoreType.DMA((2, UP_SLOTS)),
                ],
            ),
            out_shape=[jax.ShapeDtypeStruct((n_local, ROW_PIECE, d_ff), jnp.bfloat16)] * 3,
            compiler_params=pltpu.CompilerParams(dimension_semantics=("arbitrary",), vmem_limit_bytes=VMEM_LIMIT),
            cost_estimate=pl.CostEstimate(flops=4 * n_local * 192 * d_model * d_ff, bytes_accessed=4 * n_local * d_model * d_ff, transcendentals=0),
            name="experts_up",
        )(off, n_rows, at1, at2, pick, tokens, x_sib, *x_far, *x_far_sib, expert_w1, expert_w3)

        widths = [d_model * share // sum(COLUMN_SHARES) for share in COLUMN_SHARES]
        starts = [sum(widths[:chunk]) for chunk in range(len(widths))]

        def down(chunk, held):
            n_cols = widths[chunk]
            slots = 3 if n_cols > d_model // 2 else DOWN_SLOTS
            return pl.pallas_call(
                functools.partial(down_kernel, cap, starts[chunk]),
                grid_spec=pltpu.PrefetchScalarGridSpec(
                    num_scalar_prefetch=4,
                    grid=(n_local,),
                    in_specs=[any_space] * 5,
                    out_specs=[pl.BlockSpec((2, n_tok, n_cols), lambda e, *_: (0, 0, 0), **whole) for _ in range(2)],
                    scratch_shapes=[
                        pltpu.VMEM((rows, n_cols), jnp.bfloat16),
                        pltpu.VMEM((4, n_queue, n_cols), jnp.bfloat16),
                        pltpu.VMEM((slots, d_ff, n_cols), jnp.bfloat16),
                        pltpu.VMEM((slots, rows, d_ff), jnp.bfloat16),
                        pltpu.VMEM(gate_tiles.shape, jnp.bfloat16),
                        pltpu.SemaphoreType.DMA((slots,)),
                        pltpu.SemaphoreType.DMA((3, slots)),
                        pltpu.SemaphoreType.DMA((4 * n_tiles,)),
                    ],
                ),
                out_shape=[jax.ShapeDtypeStruct((2, n_tok, n_cols), jnp.float32) for _ in range(2)],
                compiler_params=pltpu.CompilerParams(dimension_semantics=("arbitrary",), vmem_limit_bytes=VMEM_LIMIT),
                cost_estimate=pl.CostEstimate(flops=2 * n_local * 192 * n_cols * d_ff, bytes_accessed=2 * n_local * n_cols * d_ff, transcendentals=0),
            )(off, n_rows, queue_off.reshape(-1), total, *held, expert_w2, gate_tiles)

        gathered = lax.all_gather(tokens, "tp", axis=0, tiled=True)
        sums_own, sums_sib, returned = [], [], []
        for chunk in range(len(widths)):
            own, sib = down(chunk, hidden)
            from_sib = swap(sib, 1)
            if chunk == 0:
                gathered, own = lax.optimization_barrier((gathered, own))
                pre_gate = jnp.dot(gathered, shared_w1, preferred_element_type=jnp.float32)
                pre_up = jnp.dot(gathered, shared_w3, preferred_element_type=jnp.float32)
                shared_hidden = (jax.nn.silu(pre_gate) * pre_up).astype(jnp.bfloat16)
                shared_hidden, *hidden = lax.optimization_barrier((shared_hidden, *hidden))
                hidden_blocks = lax.all_to_all(shared_hidden.reshape(mesh.shape["tp"], n_tok, -1), "tp", 0, 0)
            passed_on = own[1] + from_sib[1]
            returned.append(swap(passed_on, 2))
            sums_own.append(own[0])
            sums_sib.append(from_sib[0])

        width = shared_w2.shape[0]
        rep = lax.axis_index("data") * ep_size + me
        w2_part = lax.dynamic_slice_in_dim(shared_w2, rep * (width // n_rep), width // n_rep, 0)
        w2_all = lax.all_gather(w2_part, ("tp", "data", "ep"), axis=0, tiled=True)
        w2_all, passed_on = lax.optimization_barrier((w2_all, passed_on))
        w2_blocks = w2_all.reshape(mesh.shape["tp"], width, d_model)
        shared_out = jnp.einsum("sth,shd->td", hidden_blocks, w2_blocks, preferred_element_type=jnp.float32)
        base = tokens.astype(jnp.float32) + shared_out
        parts = []
        for chunk, (first, n_cols) in enumerate(zip(starts, widths)):
            routed = sums_own[chunk] + sums_sib[chunk] + returned[chunk]
            parts.append((base[:, first : first + n_cols] + routed).astype(jnp.bfloat16))
        return jnp.concatenate(parts, axis=1)


    return jax.shard_map(
        layer_body,
        mesh=mesh,
        in_specs=(row_spec, row_spec, row_spec, row_spec, row_spec, P(None, "tp"), P(None, "tp"), P("tp", None), expert_spec, expert_spec, expert_spec),
        out_specs=row_spec,
        check_vma=False,
    )
```

```python
import functools

import jax
import jax.numpy as jnp
from jax import lax
from jax.experimental import pallas as pl
from jax.experimental.pallas import tpu as pltpu
from jax.sharding import PartitionSpec as P


CAP_FACTOR = 4
GROUP = 4
COLUMN_SHARES = (3, 1)
TOKEN_SHARES = (3, 1)
ROW_PIECE = 128
UP_SLOTS = 3
DOWN_SLOTS = 4
VMEM_LIMIT = 66_000_000


def capacity_rows(n_tok, top_k, n_exp):
    return min(n_tok, ((CAP_FACTOR * n_tok * top_k // n_exp + 7) // 8) * 8)


def row_sizes(rows):
    return [size for size in (64, 128, 256) if size < rows] + [rows]


def pick_rows(n_rows, rows, body):
    low = 0
    for size in row_sizes(rows):
        high = size if size < rows else rows + 1
        pl.when((n_rows > low if low else n_rows >= 0) & (n_rows <= high))(functools.partial(body, size))
        low = size


def column_pieces(width, step):
    pieces, start = [], 0
    while start < width:
        size = min(step, width - start)
        pieces.append((start, size))
        start += size
    return pieces


def prep_kernel(total_ref, facts_ref, gates_in_ref, pick_ref, gates_ref):
    top_k = gates_in_ref.shape[2]
    n_tok = pick_ref.shape[2]
    step_rows = 32

    def fill(block, carry):
        at = pl.multiple_of(block * step_rows, step_rows)
        row = lax.broadcasted_iota(jnp.int32, (step_rows, n_tok), 0) + at
        chosen = jnp.zeros((step_rows, n_tok), jnp.float32)
        for j in range(top_k):
            chosen = jnp.where(facts_ref[0, j : j + 1, :] == row, 1.0, chosen)
        pick_ref[0, pl.ds(at, step_rows), :] = chosen.astype(jnp.bfloat16)
        return carry

    lax.fori_loop(0, pick_ref.shape[1] // step_rows, fill, 0)

    def tile(index, carry):
        row = lax.broadcasted_iota(jnp.int32, (256, n_tok), 0) + index * 256
        weights = [jnp.zeros((256, n_tok), jnp.float32) for _ in range(3)]
        for j in range(top_k):
            here = facts_ref[0, 8 + j : 9 + j, :] == row
            weights = [jnp.where(here, gates_in_ref[piece, 0, j : j + 1, :], weight) for piece, weight in enumerate(weights)]
        for piece, weight in enumerate(weights):
            gates_ref[index, piece] = weight.astype(jnp.bfloat16).T
        return carry

    lax.fori_loop(0, (total_ref[pl.program_id(0)] + 255) // 256, tile, 0)


def up_kernel(cap, off_ref, n_ref, at1_ref, at2_ref, pick_ref, x0_ref, x1_ref, x2a_ref, x2b_ref, x3a_ref, x3b_ref, w1_hbm, w3_hbm, h0_ref, h1_ref, h2_ref, rows_ref, w1_ring, w3_ring, sems):
    step = pl.program_id(0)
    n_steps = pl.num_programs(0)
    d_model = x0_ref.shape[1]
    d_ff = w1_ring.shape[2]
    n_slots = w1_ring.shape[0]
    x_refs = ((x0_ref,), (x1_ref,), (x2a_ref, x2b_ref), (x3a_ref, x3b_ref))
    piece_step = min(512, d_model // sum(TOKEN_SHARES))
    h_refs = (h0_ref, h1_ref, h2_ref)

    def fetch(expert):
        slot = expert % n_slots
        return (
            pltpu.make_async_copy(w1_hbm.at[expert], w1_ring.at[slot], sems.at[0, slot]),
            pltpu.make_async_copy(w3_hbm.at[expert], w3_ring.at[slot], sems.at[1, slot]),
        )

    def start(expert):
        for copy in fetch(expert):
            copy.start()

    @pl.when(step == 0)
    def _():
        for expert in range(n_slots - 1):
            start(expert)

    @pl.when(step + n_slots - 1 < n_steps)
    def _():
        start(step + n_slots - 1)

    @pl.when(step % GROUP == 0)
    def _():
        for src, pieces in enumerate(x_refs):
            chosen = pick_ref[src]
            base = 0
            for x_ref in pieces:
                for begin, size in column_pieces(x_ref.shape[1], piece_step):
                    got = jnp.dot(chosen, x_ref[:, begin : begin + size], preferred_element_type=jnp.float32).astype(jnp.bfloat16)
                    for part in range(GROUP):
                        at = pl.multiple_of(off_ref[(step + part) * 4 + src], 16)
                        rows_ref[part, pl.ds(at, cap), base + begin : base + begin + size] = got[part * cap : (part + 1) * cap]
                base += x_ref.shape[1]

    part = step % GROUP
    slot = step % n_slots
    for copy in fetch(step):
        copy.wait()

    def body(size):
        x = rows_ref[part, :size, :]

        def put(value, begin, width):
            for piece in range(-(-size // ROW_PIECE)):
                part_rows = min(size - piece * ROW_PIECE, ROW_PIECE)
                h_refs[piece][0, :part_rows, begin : begin + width] = value[piece * ROW_PIECE : piece * ROW_PIECE + part_rows]

        full = d_ff // 256 * 256
        for begin, width in column_pieces(full, 512):
            gate = jnp.dot(x, w1_ring[slot, :, begin : begin + width], preferred_element_type=jnp.float32)
            up = jnp.dot(x, w3_ring[slot, :, begin : begin + width], preferred_element_type=jnp.float32)
            put((jax.nn.silu(gate) * up).astype(jnp.bfloat16), begin, width)
        if full < d_ff:
            tail = d_ff - full
            both = jnp.concatenate([w1_ring[slot, :, full:], w3_ring[slot, :, full:]], axis=1)
            pair = jnp.dot(x, both, preferred_element_type=jnp.float32)
            put((jax.nn.silu(pair[:, :tail]) * pair[:, tail:]).astype(jnp.bfloat16), full, tail)

    pick_rows(n_ref[step], rows_ref.shape[1], body)


def down_kernel(cap, first, off_ref, n_ref, queue_off_ref, total_ref, h0_hbm, h1_hbm, h2_hbm, w2_hbm, gates_hbm, own_ref, sib_ref, out_ref, queue_ref, w2_ring, h_ring, gates_ref, w_sems, h_sems, gate_sems):
    step = pl.program_id(0)
    n_local = pl.num_programs(0)
    n_slots, _, width_all = w2_ring.shape
    n_tiles_max = gates_ref.shape[0] // 4
    h_hbm = (h0_hbm, h1_hbm, h2_hbm)

    def fetch(expert, act):
        slot = expert % n_slots
        for piece, source in enumerate(h_hbm):
            into = h_ring.at[slot, piece * ROW_PIECE : (piece + 1) * ROW_PIECE]
            copy = pltpu.make_async_copy(source.at[expert], into, h_sems.at[piece, slot])
            pl.when(n_ref[expert] > piece * ROW_PIECE)(functools.partial(act, copy))
        act(pltpu.make_async_copy(w2_hbm.at[expert, :, first : first + width_all], w2_ring.at[slot], w_sems.at[slot]))

    def gate_copies(act):
        for src in range(4):
            for tile in range(n_tiles_max):
                index = src * n_tiles_max + tile
                copy = pltpu.make_async_copy(gates_hbm.at[index], gates_ref.at[index], gate_sems.at[index])
                pl.when(tile * 256 < total_ref[src])(functools.partial(act, copy))

    @pl.when(step == 0)
    def _():
        for expert in range(n_slots - 1):
            fetch(expert, lambda copy: copy.start())

    @pl.when(step + n_slots - 1 < n_local)
    def _():
        fetch(step + n_slots - 1, lambda copy: copy.start())

    @pl.when(step == 0)
    def _():
        gate_copies(lambda copy: copy.start())

    fetch(step, lambda copy: copy.wait())
    slot = step % n_slots

    def body(size):
        h = h_ring[slot, :size, :]
        for begin, width in column_pieces(width_all, 512):
            out = jnp.dot(h, w2_ring[slot, :, begin : begin + width], preferred_element_type=jnp.float32)
            out_ref[:size, begin : begin + width] = out.astype(jnp.bfloat16)

    pick_rows(n_ref[step], out_ref.shape[0], body)
    for src in range(4):
        at = pl.multiple_of(off_ref[step * 4 + src], 16)
        to = pl.multiple_of(queue_off_ref[src * n_local + step], 16)
        end = off_ref[step * 4 + src + 1] if src < 3 else n_ref[step]

        def keep(size, at=at, to=to, src=src):
            queue_ref[src, pl.ds(to, size), :] = out_ref[pl.ds(at, size), :]

        few = min(32, cap)
        pl.when(end - at <= few)(functools.partial(keep, few))
        pl.when(end - at > few)(functools.partial(keep, cap))

    @pl.when(step == n_local - 1)
    def _():
        gate_copies(lambda copy: copy.wait())
        for src in range(4):
            total = total_ref[src]
            n_tiles = (total + 255) // 256

            def clear(piece, carry):
                at = pl.multiple_of(total + piece * 16, 16)
                queue_ref[src, pl.ds(at, 16), :] = jnp.zeros((16, width_all), jnp.bfloat16)
                return carry

            lax.fori_loop(0, (n_tiles * 256 - total) // 16, clear, 0)
            into = (own_ref, sib_ref, own_ref, sib_ref)[src]
            place = src // 2
            into[place] = jnp.zeros(into.shape[1:], jnp.float32)

            def add(tile, carry):
                at = pl.multiple_of(tile * 256, 256)
                for begin, width in column_pieces(width_all, 512):
                    held = queue_ref[src, pl.ds(at, 256), begin : begin + width]
                    new = into[place, :, begin : begin + width]
                    for piece in range(3):
                        new += jnp.dot(gates_ref[src * n_tiles_max + tile, piece], held, preferred_element_type=jnp.float32)
                    into[place, :, begin : begin + width] = new
                return carry

            lax.fori_loop(0, n_tiles, add, 0)


def solution(mesh):
    ep_size = mesh.shape["ep"]
    row_spec = P(("data", "ep", "tp"), None)
    expert_spec = P("ep", None, None)
    n_rep = mesh.shape["data"] * ep_size

    def layer_body(tokens, expert_ids, gate_vals, slot_ids, send_counts, shared_w1, shared_w3, shared_w2, expert_w1, expert_w3, expert_w2):
        n_tok, d_model = tokens.shape
        top_k = expert_ids.shape[1]
        n_local, _, d_ff = expert_w1.shape
        n_exp = n_local * ep_size
        cap = capacity_rows(n_tok, top_k, n_exp)
        rows = ep_size * cap
        n_queue = n_local * cap
        me = lax.axis_index("ep")

        def swap(value, bit):
            return lax.ppermute(value, "ep", [(i, i ^ bit) for i in range(ep_size)])

        x_far, x_far_sib, begin = [], [], 0
        for share in TOKEN_SHARES:
            size = d_model * share // sum(TOKEN_SHARES)
            x_far.append(swap(tokens[:, begin : begin + size], 2))
            x_far_sib.append(swap(x_far[-1], 1))
            begin += size
        x_sib = swap(tokens, 1)
        all_ids = jnp.arange(n_exp, dtype=jnp.int32)
        row_limit = jnp.sum(jnp.where(expert_ids[:, :, None] == all_ids, send_counts[0], 0), axis=-1)
        kept_mask = (slot_ids >= 0) & (slot_ids < row_limit)
        dest_row = jnp.where(kept_mask, expert_ids * cap + slot_ids, -1)
        facts = jnp.concatenate(
            [
                dest_row.astype(jnp.float32).T,
                jnp.where(kept_mask, gate_vals, 0.0).T,
                jnp.pad(send_counts.astype(jnp.float32), ((0, 0), (0, n_tok - n_exp))),
                jnp.zeros((15 - 2 * top_k, n_tok), jnp.float32),
            ],
            axis=0,
        )
        facts_far = swap(facts, 2)
        facts_sib = swap(facts, 1)
        facts_all = jnp.stack([facts, facts_sib, facts_far, swap(facts_far, 1)])

        dest_all = facts_all[:, :top_k].astype(jnp.int32) - me * n_queue
        dest_all = jnp.where((dest_all >= 0) & (dest_all < n_queue), dest_all, -1)
        gates_all = facts_all[:, top_k : 2 * top_k]
        counts_all = lax.dynamic_slice_in_dim(facts_all[:, 2 * top_k], me * n_local, n_local, 1).astype(jnp.int32)
        padded = (counts_all + 15) // 16 * 16
        local = jnp.arange(n_local, dtype=jnp.int32)
        before = local[None, :] < local[:, None]
        queue_off = jnp.sum(jnp.where(before[None], padded[:, None, :], 0), axis=2)
        total = jnp.sum(padded, axis=1)
        src = jnp.arange(4, dtype=jnp.int32)
        off = jnp.sum(jnp.where((src[None, :] < src[:, None])[None], padded.T[:, None, :], 0), axis=2).reshape(-1)
        n_rows = jnp.sum(padded, axis=0)

        def piece_home(piece):
            need = n_rows > piece * ROW_PIECE
            last = jnp.max(jnp.where(need[None, :] & (local[None, :] <= local[:, None]), local[None, :], -1), axis=1)
            first = jnp.min(jnp.where(need, local, n_local))
            return jnp.where(last >= 0, last, jnp.where(first < n_local, first, 0))

        at1, at2 = piece_home(1), piece_home(2)
        shift = jnp.sum(jnp.where((dest_all // cap)[..., None] == local, (queue_off - local * cap)[:, None, None, :], 0), axis=-1)
        queue_row = jnp.where(dest_all >= 0, dest_all + shift, -1)
        pad_rows = jnp.full((4, 8 - top_k, n_tok), -1, jnp.int32)
        places = jnp.concatenate([dest_all, pad_rows, queue_row, pad_rows], axis=1)
        high = lax.reduce_precision(gates_all, 8, 7)
        middle = lax.reduce_precision(gates_all - high, 8, 7)
        low = lax.reduce_precision(gates_all - high - middle, 8, 7)
        n_tiles = n_queue // 256
        places, off, n_rows, at1, at2, queue_off = lax.optimization_barrier((places, off, n_rows, at1, at2, queue_off.reshape(-1)))
        pick, gate_tiles = pl.pallas_call(
            prep_kernel,
            grid_spec=pltpu.PrefetchScalarGridSpec(
                num_scalar_prefetch=1,
                grid=(4,),
                in_specs=[
                    pl.BlockSpec((1, 16, n_tok), lambda s, *_: (s, 0, 0)),
                    pl.BlockSpec((3, 1, top_k, n_tok), lambda s, *_: (0, s, 0, 0)),
                ],
                out_specs=[
                    pl.BlockSpec((1, n_queue, n_tok), lambda s, *_: (s, 0, 0)),
                    pl.BlockSpec((n_tiles, 3, n_tok, 256), lambda s, *_: (s, 0, 0, 0)),
                ],
            ),
            out_shape=[
                pltpu.HBM((4, n_queue, n_tok), jnp.bfloat16),
                pltpu.HBM((4 * n_tiles, 3, n_tok, 256), jnp.bfloat16),
            ],
            compiler_params=pltpu.CompilerParams(dimension_semantics=("arbitrary",), vmem_limit_bytes=40_000_000),
            cost_estimate=pl.CostEstimate(flops=10**9, bytes_accessed=4 * n_queue * n_tok * 8, transcendentals=0),
            name="prep",
        )(total, places, jnp.stack([high, middle, low]))

        whole = dict(pipeline_mode=pl.Buffered(1))
        any_space = pl.BlockSpec(memory_space=pl.ANY)
        hidden = pl.pallas_call(
            functools.partial(up_kernel, cap),
            grid_spec=pltpu.PrefetchScalarGridSpec(
                num_scalar_prefetch=4,
                grid=(n_local,),
                in_specs=[
                    pl.BlockSpec((4, GROUP * cap, n_tok), lambda e, *_: (0, e // GROUP, 0)),
                    *[pl.BlockSpec(x.shape, lambda e, *_: (0, 0), **whole) for x in (tokens, x_sib, *x_far, *x_far_sib)],
                    any_space,
                    any_space,
                ],
                out_specs=[
                    pl.BlockSpec((1, ROW_PIECE, d_ff), lambda e, off, n, at1, at2: (e, 0, 0)),
                    pl.BlockSpec((1, ROW_PIECE, d_ff), lambda e, off, n, at1, at2: (at1[e], 0, 0)),
                    pl.BlockSpec((1, ROW_PIECE, d_ff), lambda e, off, n, at1, at2: (at2[e], 0, 0)),
                ],
                scratch_shapes=[
                    pltpu.VMEM((GROUP, rows, d_model), jnp.bfloat16),
                    pltpu.VMEM((UP_SLOTS, d_model, d_ff), jnp.bfloat16),
                    pltpu.VMEM((UP_SLOTS, d_model, d_ff), jnp.bfloat16),
                    pltpu.SemaphoreType.DMA((2, UP_SLOTS)),
                ],
            ),
            out_shape=[jax.ShapeDtypeStruct((n_local, ROW_PIECE, d_ff), jnp.bfloat16)] * 3,
            compiler_params=pltpu.CompilerParams(dimension_semantics=("arbitrary",), vmem_limit_bytes=VMEM_LIMIT),
            cost_estimate=pl.CostEstimate(flops=4 * n_local * 192 * d_model * d_ff, bytes_accessed=4 * n_local * d_model * d_ff, transcendentals=0),
            name="experts_up",
        )(off, n_rows, at1, at2, pick, tokens, x_sib, *x_far, *x_far_sib, expert_w1, expert_w3)

        widths = [d_model * share // sum(COLUMN_SHARES) for share in COLUMN_SHARES]
        starts = [sum(widths[:chunk]) for chunk in range(len(widths))]

        def down(chunk, held):
            n_cols = widths[chunk]
            slots = 3 if n_cols > d_model // 2 else DOWN_SLOTS
            return pl.pallas_call(
                functools.partial(down_kernel, cap, starts[chunk]),
                grid_spec=pltpu.PrefetchScalarGridSpec(
                    num_scalar_prefetch=4,
                    grid=(n_local,),
                    in_specs=[any_space] * 5,
                    out_specs=[pl.BlockSpec((2, n_tok, n_cols), lambda e, *_: (0, 0, 0), **whole) for _ in range(2)],
                    scratch_shapes=[
                        pltpu.VMEM((rows, n_cols), jnp.bfloat16),
                        pltpu.VMEM((4, n_queue, n_cols), jnp.bfloat16),
                        pltpu.VMEM((slots, d_ff, n_cols), jnp.bfloat16),
                        pltpu.VMEM((slots, rows, d_ff), jnp.bfloat16),
                        pltpu.VMEM(gate_tiles.shape, jnp.bfloat16),
                        pltpu.SemaphoreType.DMA((slots,)),
                        pltpu.SemaphoreType.DMA((3, slots)),
                        pltpu.SemaphoreType.DMA((4 * n_tiles,)),
                    ],
                ),
                out_shape=[jax.ShapeDtypeStruct((2, n_tok, n_cols), jnp.float32) for _ in range(2)],
                compiler_params=pltpu.CompilerParams(dimension_semantics=("arbitrary",), vmem_limit_bytes=VMEM_LIMIT),
                cost_estimate=pl.CostEstimate(flops=2 * n_local * 192 * n_cols * d_ff, bytes_accessed=2 * n_local * n_cols * d_ff, transcendentals=0),
            )(off, n_rows, queue_off, total, *held, expert_w2, gate_tiles)

        gathered = lax.all_gather(tokens, "tp", axis=0, tiled=True)
        sums_own, sums_sib, returned = [], [], []
        for chunk in range(len(widths)):
            own, sib = down(chunk, hidden)
            from_sib = swap(sib, 1)
            if chunk == 0:
                gathered, own = lax.optimization_barrier((gathered, own))
                pre_gate = jnp.dot(gathered, shared_w1, preferred_element_type=jnp.float32)
                pre_up = jnp.dot(gathered, shared_w3, preferred_element_type=jnp.float32)
                shared_hidden = (jax.nn.silu(pre_gate) * pre_up).astype(jnp.bfloat16)
                shared_hidden, *hidden = lax.optimization_barrier((shared_hidden, *hidden))
                hidden_blocks = lax.all_to_all(shared_hidden.reshape(mesh.shape["tp"], n_tok, -1), "tp", 0, 0)
            passed_on = own[1] + from_sib[1]
            returned.append(swap(passed_on, 2))
            sums_own.append(own[0])
            sums_sib.append(from_sib[0])

        width = shared_w2.shape[0]
        rep = lax.axis_index("data") * ep_size + me
        w2_part = lax.dynamic_slice_in_dim(shared_w2, rep * (width // n_rep), width // n_rep, 0)
        w2_all = lax.all_gather(w2_part, ("tp", "data", "ep"), axis=0, tiled=True)
        w2_all, passed_on = lax.optimization_barrier((w2_all, passed_on))
        w2_blocks = w2_all.reshape(mesh.shape["tp"], width, d_model)
        shared_out = jnp.einsum("sth,shd->td", hidden_blocks, w2_blocks, preferred_element_type=jnp.float32)
        base = tokens.astype(jnp.float32) + shared_out
        parts = []
        for chunk, (first, n_cols) in enumerate(zip(starts, widths)):
            routed = sums_own[chunk] + sums_sib[chunk] + returned[chunk]
            parts.append((base[:, first : first + n_cols] + routed).astype(jnp.bfloat16))
        return jnp.concatenate(parts, axis=1)


    return jax.shard_map(
        layer_body,
        mesh=mesh,
        in_specs=(row_spec, row_spec, row_spec, row_spec, row_spec, P(None, "tp"), P(None, "tp"), P("tp", None), expert_spec, expert_spec, expert_spec),
        out_specs=row_spec,
        check_vma=False,
    )
```
